256 devices in a mesh: nodes: 128 (over y, z, x), feat: 2 (over core).
Axes of the slice: x: 4, y: 4, z: 8, core: 2. Of those that a mesh axis runs over, the one named last changes fastest.
Arguments:
- features: bfloat16 [65536, 128], P('nodes'), may hold values from -6 to 6
- row_counts: int32 [128], P('nodes'), may hold values from 128 to 512, as said below
- send_rows: int32 [128, 128, 64], P('nodes'), may hold values from 0 to 511, as said below
- edge_src: int32 [2, 524288], P(None, 'nodes'), may hold values from 0 to 8703, as said below
- edge_dst: int32 [2, 524288], P(None, 'nodes'), may hold values from 0 to 511, as said below
- edge_keep: int32 [2, 524288], P(None, 'nodes'), may hold values 0 or 1
- w_first: bfloat16 [128, 512], P(None, 'feat'), may hold values from -0.5 to 0.5
- b_first: float32 [512], P('feat'), may hold values from -3 to 3
- w_second: bfloat16 [512, 512], P(None, 'feat'), may hold values from -0.25 to 0.25
Outputs:
- normed: bfloat16 [2, 65536, 512], P(None, 'nodes', 'feat')
- correlation: float32 [512, 512], P('nodes', 'feat')
- barlow_loss: float32 [], replicated
The draws below stay inside these ranges and needn't reach their ends.
Inputs may be any that keep to these rules, and one draw needn't show every extreme that they name: `row_counts`: some partition has all 512 rows live. send_rows[i, j, h] is below row_counts[i]. `edge_src`: A source below 512 is below row_counts of the edge's partition. `edge_dst`: A partition's edge slots come in aligned blocks of 1024 slots; block k targets rows k * 128 to (k + 1) * 128 - 1.
All inputs are finite; a program needn't handle non-finite values. No bound on the sum of `edge_keep` on one device may be relied on, other than what follows from the above.
Results may differ from the reference program's by a relative error of at most 0.0017.
The reference program's roundings to bfloat16 on the way (of `hidden` and `projected`) count: a program that leaves them out, or rounds other values in their place, can miss the bound.
Values may be sent and summed in bfloat16 or wider, within the bound.
No kernel may reach another device: no remote copies, remote signals or barrier semaphores. Data moves between devices by JAX's collectives and lax.ppermute only.
A program may use at most 64 MiB of HBM per device.

```python
import jax
import jax.numpy as jnp
from jax import lax

F_IN = 128
HID = 512
EMB = 512
ROWS_DEV = 512
HALO = 64
TILE_ROWS = 128
PARTITIONS = 128
EDGES_DEV = 4096
NODES = 65536


def shared_counts(key):
    folded = jax.random.fold_in(key, 11)
    first_key, second_key = jax.random.split(folded)
    counts = jax.random.randint(first_key, (PARTITIONS,), ROWS_DEV // 4, ROWS_DEV + 1)
    full_part = jax.random.randint(second_key, (), 0, PARTITIONS)
    return jnp.where(jnp.arange(PARTITIONS) == full_part, ROWS_DEV, counts).astype(jnp.int32)


def draw_row_counts(key, part):
    return shared_counts(key)


def draw_send_rows(key, part):
    counts = shared_counts(key)
    folded = jax.random.fold_in(key, 21)
    return jax.random.randint(folded, (PARTITIONS, PARTITIONS, HALO), 0, counts[:, None, None]).astype(jnp.int32)


def draw_edge_src(key, part):
    counts = shared_counts(key)
    folded = jax.random.fold_in(key, 31)
    local_key, remote_key, pick_key = jax.random.split(folded, 3)
    shape = (2, PARTITIONS, EDGES_DEV)
    local_src = jax.random.randint(local_key, shape, 0, counts[None, :, None])
    remote_src = ROWS_DEV + jax.random.randint(remote_key, shape, 0, PARTITIONS * HALO)
    pick = jax.random.randint(pick_key, shape, 0, 2)
    return jnp.where(pick == 1, remote_src, local_src).reshape(2, PARTITIONS * EDGES_DEV).astype(jnp.int32)


def draw_edge_dst(key, part):
    folded = jax.random.fold_in(key, 41)
    tiles = ROWS_DEV // TILE_ROWS
    shape = (2, PARTITIONS, tiles, EDGES_DEV // tiles)
    offsets = jax.random.randint(folded, shape, 0, TILE_ROWS)
    bases = (jnp.arange(tiles, dtype=jnp.int32) * TILE_ROWS)[None, None, :, None]
    return (offsets + bases).reshape(2, PARTITIONS * EDGES_DEV).astype(jnp.int32)


def plant(drawn, rng, low, top_value):
    spot = [jax.random.randint(jax.random.fold_in(rng, axis), (), 0, length) for axis, length in enumerate(drawn.shape)]
    main_axis = drawn.shape.index(max(drawn.shape))
    beside = spot[:main_axis] + [(spot[main_axis] + 1) % drawn.shape[main_axis]] + spot[main_axis + 1:]
    return drawn.at[tuple(spot)].set(low).at[tuple(beside)].set(top_value)


def shard_levels(own_key, dims, shards, least, high):
    def one(axis_at, parts):
        steps = jax.random.uniform(jax.random.fold_in(jax.random.fold_in(own_key, 6), axis_at), (parts,), jnp.float32, least / len(shards), high / len(shards))
        return jnp.repeat(jnp.exp(steps), dims[axis_at] // parts).reshape((-1,) + (1,) * (len(dims) - axis_at - 1))

    loudness = one(*shards[0])
    for cut in shards[1:]:
        loudness = loudness * one(*cut)
    return loudness


def normal_values(rng, extent, scale, reach, shards=(), kind=jnp.bfloat16):
    values = jax.random.normal(rng, extent, jnp.float32) * scale
    if len(shards) > 0:
        values = shard_levels(rng, extent, shards, -0.22, 0.18) * values
    return jnp.clip(values, min=-reach, max=reach).astype(kind)


def setup_inputs(seed: int = 0) -> dict:
    splits = jax.random.split(jax.random.key(seed), 10)
    features = normal_values(splits[0], (NODES, F_IN), 1.0, 6.0, ((0, 128),))
    row_counts = draw_row_counts(jax.random.fold_in(splits[9], 71), 0)
    send_rows = draw_send_rows(jax.random.fold_in(splits[9], 71), 0)
    edge_src = draw_edge_src(jax.random.fold_in(splits[9], 71), 0)
    edge_dst = draw_edge_dst(jax.random.fold_in(splits[9], 71), 0)
    edge_keep = plant((jax.random.randint(splits[5], (2, PARTITIONS * EDGES_DEV), 0, 4) < 3).astype(jnp.int32), jax.random.fold_in(splits[5], 1), 0, 1)
    w_first = normal_values(splits[6], (F_IN, HID), F_IN ** -0.5, 0.5, ((1, 2),))
    b_first = normal_values(splits[7], (HID,), 0.5, 3.0, ((0, 2),), jnp.float32)
    w_second = normal_values(splits[8], (HID, EMB), HID ** -0.5, 0.25, ((1, 2),))
    return {"features": features, "row_counts": row_counts, "send_rows": send_rows, "edge_src": edge_src, "edge_dst": edge_dst, "edge_keep": edge_keep, "w_first": w_first, "b_first": b_first, "w_second": w_second}


def reference(features, row_counts, send_rows, edge_src, edge_dst, edge_keep, w_first, b_first, w_second):
    partitions = row_counts.shape[0]
    local_rows = features.shape[0] // partitions
    edge_total = edge_src.shape[1] // partitions
    kept_edges = edge_keep.astype(jnp.float32)
    slot_index = jnp.arange(local_rows, dtype=jnp.int32)
    live_rows = (slot_index[None, :] < row_counts[:, None]).reshape(-1).astype(jnp.float32)[:, None]

    def mix_view(lookup, view_index):

        def per_part(part_index):
            local_block = lax.dynamic_slice_in_dim(lookup, part_index * local_rows, local_rows, 0)
            sender_base = jnp.arange(partitions, dtype=jnp.int32)[:, None] * local_rows
            inbound = (sender_base + lax.dynamic_index_in_dim(send_rows, part_index, 1, False)).reshape(-1).astype(jnp.int32)
            combined = jnp.concatenate([local_block, lookup[inbound]], 0).astype(jnp.float32)
            sources = lax.dynamic_slice_in_dim(edge_src[view_index], part_index * edge_total, edge_total, 0)
            targets = lax.dynamic_slice_in_dim(edge_dst[view_index], part_index * edge_total, edge_total, 0)
            weights = lax.dynamic_slice_in_dim(kept_edges[view_index], part_index * edge_total, edge_total, 0)
            summed = jax.ops.segment_sum(combined[sources] * weights[:, None], targets, num_segments=local_rows)
            degree = jax.ops.segment_sum(weights, targets, num_segments=local_rows)
            return (combined[:local_rows] + summed) / (1.0 + degree)[:, None]
        stacked = lax.map(per_part, jnp.arange(partitions, dtype=jnp.int32))
        return stacked.reshape(partitions * local_rows, -1)
    proj = jnp.dot(features, w_first, preferred_element_type=jnp.float32)
    live_count = jnp.sum(row_counts).astype(jnp.float32)
    normed_list = []
    for view_index in range(2):
        hidden = jax.nn.relu(mix_view(proj, view_index) + b_first).astype(jnp.bfloat16)
        projected = jnp.dot(hidden, w_second, preferred_element_type=jnp.float32).astype(jnp.bfloat16)
        embedded = mix_view(projected, view_index)
        average = lax.optimization_barrier(jnp.sum(embedded * live_rows, 0)) / live_count
        centered = (embedded - average) * live_rows
        variance = lax.optimization_barrier(jnp.sum(jnp.square(centered), 0)) / live_count
        normed_list.append((centered / jnp.sqrt(variance + 1e-05)).astype(jnp.bfloat16))
    normed = jnp.stack(normed_list)
    correlation = jnp.dot(normed[0].T, normed[1], preferred_element_type=jnp.float32) / live_count
    width = correlation.shape[0]
    diagonal = jnp.arange(width, dtype=jnp.int32)[:, None] == jnp.arange(width, dtype=jnp.int32)[None, :]
    barlow_loss = jnp.sum(jnp.where(diagonal, jnp.square(1.0 - correlation), 0.005 * jnp.square(correlation)))
    return (normed, correlation, barlow_loss)
```

```python
import functools

import jax
import jax.numpy as jnp
from jax import lax
from jax.experimental import pallas as pl
from jax.experimental.pallas import tpu as pltpu
from jax.sharding import Mesh
from jax.sharding import PartitionSpec as P

NODES = ("nodes_0", "nodes_1", "nodes_2")
NODES_FEAT = ("nodes_0", "nodes_1", "nodes_2", "feat")

LANES = 128
TILE = 128
CODE_BITS = 19
CODE_TOP = 2 ** (CODE_BITS - 1)
SCALE_BIAS = 224.0

VMEM = pl.BlockSpec(memory_space=pltpu.VMEM)
SMEM = pl.BlockSpec(memory_space=pltpu.SMEM)


def call(body, outs, scratch, *operands, scalars=(), name):
    return pl.pallas_call(
        body,
        out_shape=outs,
        in_specs=[SMEM] * len(scalars) + [VMEM] * len(operands),
        out_specs=jax.tree.map(lambda _: VMEM, outs),
        scratch_shapes=scratch,
        compiler_params=pltpu.CompilerParams(vmem_limit_bytes=56 * 2**20),
        name=name,
    )(*scalars, *operands)


def pick_rows(index, first_index, table, rows, first_row, count, unroll):
    def step(block, _):
        base = pl.multiple_of(block * unroll, unroll)
        for lane in range(unroll):
            source = index[first_index + base + lane]
            rows[pl.ds(first_row + base + lane, 1), :] = table[pl.ds(source, 1), :]
        return 0

    lax.fori_loop(0, count // unroll, step, 0)


def in_chunks(total, size, body):
    def step(block, _):
        body(pl.multiple_of(block * size, size))
        return 0

    lax.fori_loop(0, total // size, step, 0)


def several(total, unroll, body):
    def step(block, _):
        for one in range(unroll):
            body(block * unroll + one)
        return 0

    lax.fori_loop(0, total // unroll, step, 0)


def edge_table(targets, tile):
    inside = targets[tile : tile + 1, :] - tile * TILE
    row = lax.broadcasted_iota(jnp.int32, (TILE, targets.shape[1]), 0)
    table = jnp.where(inside == row, 1.0, 0.0)
    return table.astype(jnp.bfloat16), jnp.sum(table, 1, keepdims=True)


def send_features(core, outbound, features, out, table, rows):
    table[...] = features[...].astype(jnp.float32)
    half = out.shape[0] // LANES
    first = core[0] * half

    def step(block, _):
        base = pl.multiple_of(block * 4 * half, 4 * half)
        for peer in range(4):
            for slot in range(half):
                source = outbound[(block * 4 + peer) * (2 * half) + first + slot]
                rows[pl.ds(base + peer * half + slot, 1), :] = table[pl.ds(source, 1), :]
        return 0

    lax.fori_loop(0, out.shape[0] // (4 * half), step, 0)

    def narrow(base):
        out[pl.ds(base, 256), :] = rows[pl.ds(base, 256), :].astype(jnp.bfloat16)

    in_chunks(out.shape[0], 256, narrow)


def first_mix(
    live_count,
    sources,
    outbound,
    features,
    own,
    other,
    targets,
    mixed,
    words,
    table,
    picked,
    codes,
    coded,
):
    local = features.shape[0]
    halo = own.shape[0]
    table[0:local, :] = features[...].astype(jnp.float32)

    def widen(base):
        table[pl.ds(local + base, 256), :] = own[pl.ds(base, 256), :].astype(jnp.float32)
        table[pl.ds(local + halo + base, 256), :] = other[pl.ds(base, 256), :].astype(jnp.float32)

    in_chunks(halo, 256, widen)
    edges = targets.shape[1]
    pick_rows(sources, 0, table, picked, 0, edges * (local // TILE), 128)
    for tile in range(local // TILE):
        onehot, degree = edge_table(targets, tile)
        summed = jnp.dot(
            onehot,
            picked[tile * edges : (tile + 1) * edges, :].astype(jnp.bfloat16),
            preferred_element_type=jnp.float32,
        )
        rows = slice(tile * TILE, (tile + 1) * TILE)
        mix = (table[rows, :] + summed) / (1.0 + degree)
        mixed[rows, :] = mix
        top = jnp.maximum(jnp.max(jnp.abs(mix), 1, keepdims=True), 1e-30)
        step = jnp.clip(jnp.floor(8.0 * jnp.log2(top)) + (2.0 + SCALE_BIAS), 0.0, 255.0)
        code = jnp.round(mix * (jnp.exp2((SCALE_BIAS - step) * 0.125) * CODE_TOP))
        code = jnp.clip(code, -CODE_TOP, CODE_TOP - 1).astype(jnp.int32)
        codes[rows, :] = (code & (2**CODE_BITS - 1)) | (step.astype(jnp.int32) << CODE_BITS)

    pick_rows(outbound, 0, codes, coded, 0, coded.shape[0], 128)
    group = lax.broadcasted_iota(jnp.int32, (8, LANES), 1) // 16

    patch = lax.broadcasted_iota(jnp.int32, (8, LANES), 0)
    count = jnp.where(patch == 0, live_count[0] & 255, live_count[0] >> 8) << 24
    patched = (lax.broadcasted_iota(jnp.int32, (8, LANES), 1) == 1) & (patch < 2)

    def pack(peer):
        base = pl.multiple_of(peer * 64, 64)
        to = pl.multiple_of(peer * 40, 8)
        octet = [coded[pl.ds(base + 8 * k, 8), :] for k in range(8)]
        for k in range(4):
            low = (octet[k] >> 3) & 0xFFFF
            words[pl.ds(to + 8 * k, 8), :] = low | ((octet[k + 4] >> 3) << 16)
        rest = jnp.zeros((8, LANES), jnp.int32)
        steps = jnp.zeros((8, LANES), jnp.int32)
        for k in range(8):
            rest = rest | ((octet[k] & 7) << (3 * k))
            steps = jnp.where(group == k, octet[k], steps)
        rest = rest | jnp.where(patched, count, (steps >> CODE_BITS) << 24)
        words[pl.ds(to + 32, 8), :] = rest

    several(coded.shape[0] // 64, 8, pack)


def split_three(value):
    first = value.astype(jnp.bfloat16)
    rest = value - first.astype(jnp.float32)
    second = rest.astype(jnp.bfloat16)
    third = (rest - second.astype(jnp.float32)).astype(jnp.bfloat16)
    return first, second, third


def second_mix(
    core,
    live_count,
    sources,
    words,
    mixed,
    targets,
    w1_own,
    w1_other,
    b_own,
    b_other,
    w2_own,
    w2_other,
    embedded,
    sums,
    node_total,
    table,
    picked,
    w1,
    w2,
):
    local = mixed.shape[0]
    half = w1_own.shape[1]
    me = core[0]
    mine = pl.multiple_of(me * half, half)
    theirs = pl.multiple_of((1 - me) * half, half)
    for piece in range(3):
        w1[piece * LANES : (piece + 1) * LANES, 0:half] = w1_own[...]
        w1[piece * LANES : (piece + 1) * LANES, half : 2 * half] = w1_other[...]
    w2[0:half, 0:half] = w2_own[pl.ds(mine, half), :]
    w2[half : 2 * half, 0:half] = w2_own[pl.ds(theirs, half), :]
    w2[0:half, half : 2 * half] = w2_other[pl.ds(mine, half), :]
    w2[half : 2 * half, half : 2 * half] = w2_other[pl.ds(theirs, half), :]
    bias = jnp.concatenate([b_own[...], b_other[...]], 1)

    table[0:local, :] = mixed[...]

    def unpack(peer):
        base = pl.multiple_of(peer * 40, 8)
        to = pl.multiple_of(local + peer * 64, 64)
        pairs = [words[pl.ds(base + 8 * k, 8), :] for k in range(4)]
        rest = words[pl.ds(base + 32, 8), :]
        step = (rest >> 24) & 255
        scale = jnp.exp2((step.astype(jnp.float32) - SCALE_BIAS) * 0.125) * (1.0 / CODE_TOP)
        for k in range(8):
            high = (pairs[k] << 16) >> 16 if k < 4 else pairs[k - 4] >> 16
            code = (high << 3) | ((rest >> (3 * k)) & 7)
            table[pl.ds(to + 8 * k, 8), :] = (
                code.astype(jnp.float32) * scale[:, 16 * k : 16 * k + 1]
            )
        return step

    def unpack_several(block, counts):
        for one in range(8):
            counts = counts + unpack(block * 8 + one)
        return counts

    counts = lax.fori_loop(
        0, words.shape[0] // 320, unpack_several, jnp.zeros((8, LANES), jnp.int32)
    )
    sublane = lax.broadcasted_iota(jnp.int32, (8, LANES), 0)
    weight = jnp.where(sublane == 0, 1.0, jnp.where(sublane == 1, 256.0, 0.0))
    lane = lax.broadcasted_iota(jnp.int32, (8, LANES), 1)
    counts = jnp.where(lane == 1, counts.astype(jnp.float32) * weight, 0.0)
    counts = jnp.sum(jnp.sum(counts, 1, keepdims=True), 0, keepdims=True)
    node_total[...] = jnp.broadcast_to(counts, node_total.shape)
    edges = targets.shape[1]
    total = jnp.zeros((1, 2 * half), jnp.float32)
    squares = jnp.zeros((1, 2 * half), jnp.float32)
    for tile in range(local // TILE):
        rows = slice(tile * TILE, (tile + 1) * TILE)
        picked[0:TILE, :] = mixed[rows, :]
        pick_rows(sources, tile * edges, table, picked, TILE, edges, 128)
        value = jnp.concatenate(split_three(picked[...]), 1)
        hidden = jnp.dot(value, w1[...], preferred_element_type=jnp.float32) + bias
        hidden = jnp.maximum(hidden, 0.0).astype(jnp.bfloat16)
        projected = jnp.dot(hidden, w2[...], preferred_element_type=jnp.float32)
        projected = projected.astype(jnp.bfloat16)
        onehot, degree = edge_table(targets, tile)
        summed = jnp.dot(onehot, projected[TILE:, :], preferred_element_type=jnp.float32)
        value = (projected[0:TILE, :].astype(jnp.float32) + summed) / (1.0 + degree)
        embedded[rows, :] = value
        slot = tile * TILE + lax.broadcasted_iota(jnp.int32, (TILE, 1), 0)
        value = jnp.where(slot < live_count[0], value, 0.0)
        total = total + jnp.sum(value, 0, keepdims=True)
        squares = squares + jnp.sum(value * value, 0, keepdims=True)
    for part in range(4):
        columns = slice(part * LANES, (part + 1) * LANES)
        sums[:, part : part + 1, :] = jnp.broadcast_to(
            total[:, columns][None], (sums.shape[0], 1, LANES)
        )
        sums[:, part + 4 : part + 5, :] = jnp.broadcast_to(
            squares[:, columns][None], (sums.shape[0], 1, LANES)
        )


def normalize(live_count, sums, node_total, embedded, out):
    total = node_total[...]
    scaled = jnp.sum(sums[...], 0) / total
    mean, square = scaled[0:4, :], scaled[4:8, :]
    dev = jnp.sqrt(square - mean * mean + 1e-05)
    slot = lax.broadcasted_iota(jnp.int32, (embedded.shape[0], 1), 0)
    live = slot < live_count[0]
    for part in range(4):
        columns = slice(part * LANES, (part + 1) * LANES)
        value = (embedded[:, columns] - mean[part : part + 1, :]) / dev[part : part + 1, :]
        out[:, columns] = jnp.where(live, value, 0.0).astype(jnp.bfloat16)


def correlate(core, own, other, normed, out):
    half = normed.shape[2]
    width = 2 * half
    contract = (((0,), (0,)), ((), ()))

    def give(left, right):
        product = lax.dot_general(left, right, contract, preferred_element_type=jnp.float32)
        for pair in range(width // 8):
            near = product[pair * 8 : pair * 8 + 8, 0:LANES]
            far = product[pair * 8 : pair * 8 + 8, LANES:half]
            out[2 * pair] = jnp.concatenate([near[0:4], far[0:4]], 0)
            out[2 * pair + 1] = jnp.concatenate([near[4:8], far[4:8]], 0)

    @pl.when(core[0] == 0)
    def _():
        normed[0] = own[:, 0:half]
        normed[1] = other[:, half:width]
        give(own[...], other[:, half:width])

    @pl.when(core[0] == 1)
    def _():
        normed[0] = other[:, half:width]
        normed[1] = own[:, 0:half]
        give(other[...], own[:, 0:half])


def finish(core, node, arrived, node_total, correlation, loss):
    half = correlation.shape[1]
    summed = jnp.sum(arrived[...], 0) / node_total[...]
    value = jnp.concatenate([summed[0:4, :], summed[4:8, :]], 1)
    correlation[...] = value
    share = correlation.shape[0]
    row = lax.broadcasted_iota(jnp.int32, (share, half), 0) + node[0] * share
    column = lax.broadcasted_iota(jnp.int32, (share, half), 1) + core[0] * half
    terms = jnp.where(row == column, jnp.square(1.0 - value), 0.005 * jnp.square(value))
    terms = jnp.sum(jnp.sum(terms, 1, keepdims=True), 0, keepdims=True)
    loss[...] = jnp.broadcast_to(terms[None], loss.shape)


def per_device(
    features, row_counts, send_rows, edge_src, edge_dst, edge_keep, w_first, b_first, w_second
):
    local, f_in = features.shape
    peers, halo = send_rows.shape[1], send_rows.shape[2]
    edges = edge_src.shape[1]
    tiles = local // TILE
    half = w_first.shape[1]
    width = 2 * half
    f32, bf16, i32 = jnp.float32, jnp.bfloat16, jnp.int32
    shape = jax.ShapeDtypeStruct
    core_index = lax.axis_index("feat")
    node_index = lax.axis_index(NODES)
    core = core_index.reshape(1).astype(i32)
    node = node_index.reshape(1).astype(i32)
    swap = [(0, 1), (1, 0)]

    def partner(value):
        return lax.ppermute(value, "feat", swap)

    w1_other, w2_other = partner(w_first), partner(w_second)
    bias = b_first.reshape(1, half)
    bias_other = partner(bias)
    outbound = send_rows.reshape(peers * halo)
    sources = lax.dynamic_index_in_dim(edge_src, core_index, 0, False)
    targets = lax.dynamic_index_in_dim(edge_dst, core_index, 0, False)
    kept = lax.dynamic_index_in_dim(edge_keep, core_index, 0, False)
    targets = jnp.where(kept == 1, targets, -1).reshape(tiles, edges // tiles)

    rows_half = peers * halo // 2
    sent = call(
        send_features,
        shape((rows_half, f_in), bf16),
        [pltpu.VMEM((local, f_in), f32), pltpu.VMEM((rows_half, f_in), f32)],
        features,
        scalars=(core, outbound),
        name="send_features",
    )
    got = lax.all_to_all(
        sent.reshape(peers, halo // 2, f_in), NODES, split_axis=0, concat_axis=0, tiled=True
    )
    got_other = partner(got)
    remote = sources - local
    slot_half = (remote % halo) // (halo // 2)
    from_other = (slot_half != core_index).astype(i32)
    remote = (remote // halo) * (halo // 2) + remote % (halo // 2) + from_other * rows_half
    first_sources = jnp.where(sources < local, sources, remote + local)
    mixed, words = call(
        first_mix,
        (shape((local, f_in), f32), shape((peers * 40, f_in), i32)),
        [
            pltpu.VMEM((local + 2 * rows_half, f_in), f32),
            pltpu.VMEM((edges, f_in), f32),
            pltpu.VMEM((local, f_in), i32),
            pltpu.VMEM((peers * halo, f_in), i32),
        ],
        features,
        got.reshape(rows_half, f_in),
        got_other.reshape(rows_half, f_in),
        targets,
        scalars=(row_counts, first_sources, outbound),
        name="first_mix",
    )
    arrived = lax.all_to_all(
        words.reshape(peers, 40, f_in), NODES, split_axis=0, concat_axis=0, tiled=True
    )
    embedded, sums, node_total = call(
        second_mix,
        (
            shape((local, width), f32),
            shape((peers, 8, LANES), f32),
            shape((8, LANES), f32),
        ),
        [
            pltpu.VMEM((local + peers * halo, f_in), f32),
            pltpu.VMEM((TILE + edges // tiles, f_in), f32),
            pltpu.VMEM((3 * f_in, width), bf16),
            pltpu.VMEM((width, width), bf16),
        ],
        arrived.reshape(peers * 40, f_in),
        mixed,
        targets,
        w_first,
        w1_other,
        bias,
        bias_other,
        w_second,
        w2_other,
        scalars=(core, row_counts, sources),
        name="second_mix",
    )
    sums = lax.all_to_all(sums, NODES, split_axis=0, concat_axis=0, tiled=True)
    own = call(
        normalize,
        shape((local, width), bf16),
        [],
        sums,
        node_total,
        embedded,
        scalars=(row_counts,),
        name="normalize",
    )
    normed, partial = call(
        correlate,
        (shape((2, local, half), bf16), shape((peers, 8, LANES), f32)),
        [],
        own,
        partner(own),
        scalars=(core,),
        name="correlate",
    )
    partial = lax.all_to_all(partial, NODES, split_axis=0, concat_axis=0, tiled=True)
    devices = lax.axis_size(NODES_FEAT)
    correlation, loss = call(
        finish,
        (shape((width // peers, half), f32), shape((devices, 1, LANES), f32)),
        [],
        partial,
        node_total,
        scalars=(core, node),
        name="finish",
    )
    losses = lax.all_to_all(loss, NODES_FEAT, 0, 0, tiled=True)
    return (normed, correlation, jnp.sum(losses[:, 0, 0]))


def solution(mesh):
    torus = Mesh(
        mesh.devices.reshape(4, 8, 4, mesh.shape["feat"]), ("nodes_0", "nodes_1", "nodes_2", "feat")
    )
    placed = (
        P(NODES, None),
        P(NODES),
        P(NODES, None, None),
        P(None, NODES),
        P(None, NODES),
        P(None, NODES),
        P(None, "feat"),
        P("feat"),
        P(None, "feat"),
    )
    return jax.shard_map(
        per_device,
        mesh=torus,
        in_specs=placed,
        out_specs=(P(None, NODES, "feat"), P(NODES, "feat"), P()),
        check_vma=False,
    )
```

```python
import functools

import jax
import jax.numpy as jnp
from jax import lax
from jax.experimental import pallas as pl
from jax.experimental.pallas import tpu as pltpu
from jax.sharding import Mesh
from jax.sharding import PartitionSpec as P

NODES = ("nodes_0", "nodes_1", "nodes_2")
PLANE = ("nodes_0", "nodes_2")
PLANE_FEAT = ("nodes_0", "nodes_2", "feat")

LANES = 128
TILE = 128
CODE_BITS = 19
CODE_TOP = 2 ** (CODE_BITS - 1)
SCALE_BIAS = 224.0

VMEM = pl.BlockSpec(memory_space=pltpu.VMEM)
SMEM = pl.BlockSpec(memory_space=pltpu.SMEM)


def call(body, outs, scratch, *operands, scalars=(), name):
    return pl.pallas_call(
        body,
        out_shape=outs,
        in_specs=[SMEM] * len(scalars) + [VMEM] * len(operands),
        out_specs=jax.tree.map(lambda _: VMEM, outs),
        scratch_shapes=scratch,
        compiler_params=pltpu.CompilerParams(vmem_limit_bytes=26 * 2**20),
        name=name,
    )(*scalars, *operands)


def pick_rows(index, first_index, table, rows, first_row, count, unroll):
    def step(block, _):
        base = pl.multiple_of(block * unroll, unroll)
        for lane in range(unroll):
            source = index.at[pl.ds(lane, index.shape[0] - unroll)][first_index + base]
            rows[pl.ds(first_row + base + lane, 1), :] = table[pl.ds(source, 1), :]
        return 0

    lax.fori_loop(0, count // unroll, step, 0)


def in_chunks(total, size, body):
    def step(block, _):
        body(pl.multiple_of(block * size, size))
        return 0

    lax.fori_loop(0, total // size, step, 0)


def several(total, unroll, body):
    def step(block, _):
        for one in range(unroll):
            body(block * unroll + one)
        return 0

    lax.fori_loop(0, total // unroll, step, 0)


def edge_table(targets, tile):
    inside = targets[tile : tile + 1, :] - tile * TILE
    row = lax.broadcasted_iota(jnp.int32, (TILE, targets.shape[1]), 0)
    table = jnp.where(inside == row, 1.0, 0.0)
    return table.astype(jnp.bfloat16), jnp.sum(table, 1, keepdims=True)


def send_features(core, outbound, features, out, table, rows):
    table[...] = features[...].astype(jnp.float32)
    half = out.shape[0] // LANES
    first = core[0] * half

    def step(block, _):
        base = pl.multiple_of(block * 4 * half, 4 * half)
        for peer in range(4):
            for slot in range(half):
                near = outbound.at[pl.ds(peer * 2 * half + slot, outbound.shape[0] - 8 * half)]
                source = near[block * (8 * half) + first]
                rows[pl.ds(base + peer * half + slot, 1), :] = table[pl.ds(source, 1), :]
        return 0

    lax.fori_loop(0, out.shape[0] // (4 * half), step, 0)

    def narrow(base):
        out[pl.ds(base, 256), :] = rows[pl.ds(base, 256), :].astype(jnp.bfloat16)

    in_chunks(out.shape[0], 256, narrow)


def first_mix(
    live_count,
    sources,
    outbound,
    features,
    own,
    other,
    targets,
    mixed,
    words,
    table,
    picked,
    codes,
    coded,
):
    local = features.shape[0]
    halo = own.shape[0]
    table[0:local, :] = features[...].astype(jnp.float32)

    def widen(base):
        table[pl.ds(local + base, 256), :] = own[pl.ds(base, 256), :].astype(jnp.float32)
        table[pl.ds(local + halo + base, 256), :] = other[pl.ds(base, 256), :].astype(jnp.float32)

    in_chunks(halo, 256, widen)
    edges = targets.shape[1]
    pick_rows(sources, 0, table, picked, 0, edges * (local // TILE), 128)
    for tile in range(local // TILE):
        onehot, degree = edge_table(targets, tile)
        summed = jnp.dot(
            onehot,
            picked[tile * edges : (tile + 1) * edges, :].astype(jnp.bfloat16),
            preferred_element_type=jnp.float32,
        )
        rows = slice(tile * TILE, (tile + 1) * TILE)
        mix = (table[rows, :] + summed) / (1.0 + degree)
        mixed[rows, :] = mix
        top = jnp.maximum(jnp.max(jnp.abs(mix), 1, keepdims=True), 1e-30)
        step = jnp.clip(jnp.floor(8.0 * jnp.log2(top)) + (2.0 + SCALE_BIAS), 0.0, 255.0)
        code = jnp.round(mix * (jnp.exp2((SCALE_BIAS - step) * 0.125) * CODE_TOP))
        code = jnp.clip(code, -CODE_TOP, CODE_TOP - 1).astype(jnp.int32)
        codes[rows, :] = (code & (2**CODE_BITS - 1)) | (step.astype(jnp.int32) << CODE_BITS)

    pick_rows(outbound, 0, codes, coded, 0, coded.shape[0], 128)
    group = lax.broadcasted_iota(jnp.int32, (8, LANES), 1) // 16

    patch = lax.broadcasted_iota(jnp.int32, (8, LANES), 0)
    count = jnp.where(patch == 0, live_count[0] & 255, live_count[0] >> 8) << 24
    patched = (lax.broadcasted_iota(jnp.int32, (8, LANES), 1) == 1) & (patch < 2)

    def pack(peer):
        base = pl.multiple_of(peer * 64, 64)
        to = pl.multiple_of(peer * 40, 8)
        octet = [coded[pl.ds(base + 8 * k, 8), :] for k in range(8)]
        for k in range(4):
            low = (octet[k] >> 3) & 0xFFFF
            words[pl.ds(to + 8 * k, 8), :] = low | ((octet[k + 4] >> 3) << 16)
        rest = jnp.zeros((8, LANES), jnp.int32)
        steps = jnp.zeros((8, LANES), jnp.int32)
        for k in range(8):
            rest = rest | ((octet[k] & 7) << (3 * k))
            steps = jnp.where(group == k, octet[k], steps)
        rest = rest | jnp.where(patched, count, (steps >> CODE_BITS) << 24)
        words[pl.ds(to + 32, 8), :] = rest

    several(coded.shape[0] // 64, 8, pack)


def split_three(value):
    first = value.astype(jnp.bfloat16)
    rest = value - first.astype(jnp.float32)
    second = rest.astype(jnp.bfloat16)
    third = (rest - second.astype(jnp.float32)).astype(jnp.bfloat16)
    return first, second, third


def second_mix(
    core,
    live_count,
    sources,
    words,
    mixed,
    targets,
    w1_own,
    w1_other,
    b_own,
    b_other,
    w2_own,
    w2_other,
    embedded,
    sums,
    node_total,
    table,
    picked,
    w1,
    w2,
):
    local = mixed.shape[0]
    half = w1_own.shape[1]
    me = core[0]
    mine = pl.multiple_of(me * half, half)
    theirs = pl.multiple_of((1 - me) * half, half)
    for piece in range(3):
        w1[piece * LANES : (piece + 1) * LANES, 0:half] = w1_own[...]
        w1[piece * LANES : (piece + 1) * LANES, half : 2 * half] = w1_other[...]
    w2[0:half, 0:half] = w2_own[pl.ds(mine, half), :]
    w2[half : 2 * half, 0:half] = w2_own[pl.ds(theirs, half), :]
    w2[0:half, half : 2 * half] = w2_other[pl.ds(mine, half), :]
    w2[half : 2 * half, half : 2 * half] = w2_other[pl.ds(theirs, half), :]
    bias = jnp.concatenate([b_own[...], b_other[...]], 1)

    table[0:local, :] = mixed[...]

    def unpack(peer):
        base = pl.multiple_of(peer * 40, 8)
        to = pl.multiple_of(local + peer * 64, 64)
        pairs = [words[pl.ds(base + 8 * k, 8), :] for k in range(4)]
        rest = words[pl.ds(base + 32, 8), :]
        step = (rest >> 24) & 255
        scale = jnp.exp2((step.astype(jnp.float32) - SCALE_BIAS) * 0.125) * (1.0 / CODE_TOP)
        for k in range(8):
            high = (pairs[k] << 16) >> 16 if k < 4 else pairs[k - 4] >> 16
            code = (high << 3) | ((rest >> (3 * k)) & 7)
            table[pl.ds(to + 8 * k, 8), :] = (
                code.astype(jnp.float32) * scale[:, 16 * k : 16 * k + 1]
            )
        return step

    def unpack_several(block, counts):
        for one in range(8):
            counts = counts + unpack(block * 8 + one)
        return counts

    counts = lax.fori_loop(
        0, words.shape[0] // 320, unpack_several, jnp.zeros((8, LANES), jnp.int32)
    )
    sublane = lax.broadcasted_iota(jnp.int32, (8, LANES), 0)
    weight = jnp.where(sublane == 0, 1.0, jnp.where(sublane == 1, 256.0, 0.0))
    lane = lax.broadcasted_iota(jnp.int32, (8, LANES), 1)
    counts = jnp.where(lane == 1, counts.astype(jnp.float32) * weight, 0.0)
    counts = jnp.sum(jnp.sum(counts, 1, keepdims=True), 0, keepdims=True)
    node_total[...] = jnp.broadcast_to(counts, node_total.shape)
    edges = targets.shape[1]
    total = jnp.zeros((1, 2 * half), jnp.float32)
    squares = jnp.zeros((1, 2 * half), jnp.float32)
    for tile in range(local // TILE):
        rows = slice(tile * TILE, (tile + 1) * TILE)
        picked[0:TILE, :] = mixed[rows, :]
        pick_rows(sources, tile * edges, table, picked, TILE, edges, 128)
        value = jnp.concatenate(split_three(picked[...]), 1)
        hidden = jnp.dot(value, w1[...], preferred_element_type=jnp.float32) + bias
        hidden = jnp.maximum(hidden, 0.0).astype(jnp.bfloat16)
        projected = jnp.dot(hidden, w2[...], preferred_element_type=jnp.float32)
        projected = projected.astype(jnp.bfloat16)
        onehot, degree = edge_table(targets, tile)
        summed = jnp.dot(onehot, projected[TILE:, :], preferred_element_type=jnp.float32)
        value = (projected[0:TILE, :].astype(jnp.float32) + summed) / (1.0 + degree)
        embedded[rows, :] = value
        slot = tile * TILE + lax.broadcasted_iota(jnp.int32, (TILE, 1), 0)
        value = jnp.where(slot < live_count[0], value, 0.0)
        total = total + jnp.sum(value, 0, keepdims=True)
        squares = squares + jnp.sum(value * value, 0, keepdims=True)
    for part in range(4):
        columns = slice(part * LANES, (part + 1) * LANES)
        for peer in range(sums.shape[0]):
            sums[peer, part : part + 1, :] = total[:, columns]
            sums[peer, part + 4 : part + 5, :] = squares[:, columns]


def add_and_copy(arrived, out):
    total = arrived[0]
    for peer in range(1, arrived.shape[0]):
        total = total + arrived[peer]
    for peer in range(out.shape[0]):
        out[peer] = total


def normalize(live_count, sums, node_total, embedded, out):
    total = node_total[...]
    scaled = jnp.sum(sums[...], 0) / total
    mean, square = scaled[0:4, :], scaled[4:8, :]
    dev = jnp.sqrt(square - mean * mean + 1e-05)
    slot = lax.broadcasted_iota(jnp.int32, (embedded.shape[0], 1), 0)
    live = slot < live_count[0]
    for part in range(4):
        columns = slice(part * LANES, (part + 1) * LANES)
        value = (embedded[:, columns] - mean[part : part + 1, :]) / dev[part : part + 1, :]
        out[:, columns] = jnp.where(live, value, 0.0).astype(jnp.bfloat16)


def correlate(core, own, other, normed, out):
    half = normed.shape[2]
    width = 2 * half
    groups, depth, wide = out.shape[0], out.shape[1] // 4, 4
    contract = (((0,), (0,)), ((), ()))

    def give(left, right):
        product = lax.dot_general(left, right, contract, preferred_element_type=jnp.float32)
        for group in range(groups):
            for near in range(0, depth, 2):
                rows = []
                for n1 in (near, near + 1):
                    first = ((group // wide) * depth * wide + n1 * wide + group % wide) * 4
                    rows.append(product[first : first + 4, :])
                out[group, near * 4 : near * 4 + 8, :] = jnp.concatenate(rows, 0)

    @pl.when(core[0] == 0)
    def _():
        normed[0] = own[:, 0:half]
        normed[1] = other[:, half:width]
        give(own[...], other[:, half:width])

    @pl.when(core[0] == 1)
    def _():
        normed[0] = other[:, half:width]
        normed[1] = own[:, 0:half]
        give(other[...], own[:, 0:half])


def finish(core, node, arrived, node_total, correlation, loss):
    half = correlation.shape[1]
    share, depth, wide = 4, 8, 4
    n0, n1, n2 = node[0] // (depth * wide), (node[0] // wide) % depth, node[0] % wide
    value = arrived[0]
    for peer in range(1, arrived.shape[0]):
        value = value + arrived[peer]
    value = value / node_total[0:1, 0:1]
    place = lax.broadcasted_iota(jnp.int32, value.shape, 0)
    row = ((n0 * depth + place // share) * wide + n2) * share + place % share
    column = lax.broadcasted_iota(jnp.int32, value.shape, 1) + core[0] * half
    mine = value[0:share, :]
    for other in range(1, depth):
        mine = jnp.where(n1 == other, value[other * share : (other + 1) * share, :], mine)
    correlation[...] = mine
    terms = jnp.where(row == column, jnp.square(1.0 - value), 0.005 * jnp.square(value))
    terms = jnp.sum(jnp.sum(terms, 1, keepdims=True), 0, keepdims=True)
    loss[...] = jnp.broadcast_to(terms[None], loss.shape)


def per_device(
    features, row_counts, send_rows, edge_src, edge_dst, edge_keep, w_first, b_first, w_second
):
    local, f_in = features.shape
    peers, halo = send_rows.shape[1], send_rows.shape[2]
    edges = edge_src.shape[1]
    tiles = local // TILE
    half = w_first.shape[1]
    width = 2 * half
    f32, bf16, i32 = jnp.float32, jnp.bfloat16, jnp.int32
    shape = jax.ShapeDtypeStruct
    core_index = lax.axis_index("feat")
    node_index = lax.axis_index(NODES)
    core = core_index.reshape(1).astype(i32)
    node = node_index.reshape(1).astype(i32)
    swap = [(0, 1), (1, 0)]
    planes, depth = lax.axis_size(PLANE), lax.axis_size("nodes_1")

    def partner(value):
        return lax.ppermute(value, "feat", swap)

    def sum_over_nodes(blocks, name):
        blocks = lax.all_to_all(blocks, PLANE, split_axis=0, concat_axis=0, tiled=True)
        copies = call(
            add_and_copy, shape((depth, *blocks.shape[1:]), f32), [], blocks, name=name
        )
        return lax.all_to_all(copies, "nodes_1", split_axis=0, concat_axis=0, tiled=True)

    w1_other, w2_other = partner(w_first), partner(w_second)
    bias = b_first.reshape(1, half)
    bias_other = partner(bias)
    outbound = send_rows.reshape(peers * halo)
    sources = lax.dynamic_index_in_dim(edge_src, core_index, 0, False)
    targets = lax.dynamic_index_in_dim(edge_dst, core_index, 0, False)
    kept = lax.dynamic_index_in_dim(edge_keep, core_index, 0, False)
    targets = jnp.where(kept == 1, targets, -1).reshape(tiles, edges // tiles)

    rows_half = peers * halo // 2
    sent = call(
        send_features,
        shape((rows_half, f_in), bf16),
        [pltpu.VMEM((local, f_in), f32), pltpu.VMEM((rows_half, f_in), f32)],
        features,
        scalars=(core, outbound),
        name="send_features",
    )
    got = lax.all_to_all(
        sent.reshape(peers, halo // 2, f_in), NODES, split_axis=0, concat_axis=0, tiled=True
    )
    got_other = partner(got)
    remote = sources - local
    slot_half = (remote % halo) // (halo // 2)
    from_other = (slot_half != core_index).astype(i32)
    remote = (remote // halo) * (halo // 2) + remote % (halo // 2) + from_other * rows_half
    first_sources = jnp.where(sources < local, sources, remote + local)
    mixed, words = call(
        first_mix,
        (shape((local, f_in), f32), shape((peers * 40, f_in), i32)),
        [
            pltpu.VMEM((local + 2 * rows_half, f_in), f32),
            pltpu.VMEM((edges, f_in), f32),
            pltpu.VMEM((local, f_in), i32),
            pltpu.VMEM((peers * halo, f_in), i32),
        ],
        features,
        got.reshape(rows_half, f_in),
        got_other.reshape(rows_half, f_in),
        targets,
        scalars=(row_counts, first_sources, outbound),
        name="first_mix",
    )
    arrived = lax.all_to_all(
        words.reshape(peers, 40, f_in), NODES, split_axis=0, concat_axis=0, tiled=True
    )
    embedded, sums, node_total = call(
        second_mix,
        (
            shape((local, width), f32),
            shape((planes, 8, LANES), f32),
            shape((8, LANES), f32),
        ),
        [
            pltpu.VMEM((local + peers * halo, f_in), f32),
            pltpu.VMEM((TILE + edges // tiles, f_in), f32),
            pltpu.VMEM((3 * f_in, width), bf16),
            pltpu.VMEM((width, width), bf16),
        ],
        arrived.reshape(peers * 40, f_in),
        mixed,
        targets,
        w_first,
        w1_other,
        bias,
        bias_other,
        w_second,
        w2_other,
        scalars=(core, row_counts, sources),
        name="second_mix",
    )
    sums = sum_over_nodes(sums, "add_sums")
    own = call(
        normalize,
        shape((local, width), bf16),
        [],
        sums,
        node_total,
        embedded,
        scalars=(row_counts,),
        name="normalize",
    )
    normed, partial = call(
        correlate,
        (shape((2, local, half), bf16), shape((planes, width // planes, half), f32)),
        [],
        own,
        partner(own),
        scalars=(core,),
        name="correlate",
    )
    partial = sum_over_nodes(partial, "add_products")
    devices = lax.axis_size(PLANE_FEAT)
    correlation, loss = call(
        finish,
        (shape((width // peers, half), f32), shape((devices, 1, LANES), f32)),
        [],
        partial,
        node_total,
        scalars=(core, node),
        name="finish",
    )
    losses = lax.all_to_all(loss, PLANE_FEAT, 0, 0, tiled=True)
    return (normed, correlation, jnp.sum(losses[:, 0, 0]))


def solution(mesh):
    torus = Mesh(
        mesh.devices.reshape(4, 8, 4, mesh.shape["feat"]), ("nodes_0", "nodes_1", "nodes_2", "feat")
    )
    placed = (
        P(NODES, None),
        P(NODES),
        P(NODES, None, None),
        P(None, NODES),
        P(None, NODES),
        P(None, NODES),
        P(None, "feat"),
        P("feat"),
        P(None, "feat"),
    )
    return jax.shard_map(
        per_device,
        mesh=torus,
        in_specs=placed,
        out_specs=(P(None, NODES, "feat"), P(NODES, "feat"), P()),
        check_vma=False,
    )
```

```python
import functools

import jax
import jax.numpy as jnp
from jax import lax
from jax.experimental import pallas as pl
from jax.experimental.pallas import tpu as pltpu
from jax.sharding import Mesh
from jax.sharding import PartitionSpec as P

NODES = ("nodes_0", "nodes_1", "nodes_2")
PLANE = ("nodes_0", "nodes_2")
PLANE_FEAT = ("nodes_0", "nodes_2", "feat")

LANES = 128
TILE = 128
CODE_BITS = 19
CODE_TOP = 2 ** (CODE_BITS - 1)
SCALE_BIAS = 224.0

VMEM = pl.BlockSpec(memory_space=pltpu.VMEM)
SMEM = pl.BlockSpec(memory_space=pltpu.SMEM)


def call(body, outs, scratch, *operands, scalars=(), name):
    return pl.pallas_call(
        body,
        out_shape=outs,
        in_specs=[SMEM] * len(scalars) + [VMEM] * len(operands),
        out_specs=jax.tree.map(lambda _: VMEM, outs),
        scratch_shapes=scratch,
        compiler_params=pltpu.CompilerParams(vmem_limit_bytes=26 * 2**20),
        name=name,
    )(*scalars, *operands)


def pick_rows(index, first_index, table, rows, first_row, count, unroll):
    def step(block, _):
        base = pl.multiple_of(block * unroll, unroll)
        for lane in range(unroll):
            source = index.at[pl.ds(lane, index.shape[0] - unroll)][first_index + base]
            rows[pl.ds(first_row + base + lane, 1), :] = table[pl.ds(source, 1), :]
        return 0

    lax.fori_loop(0, count // unroll, step, 0)


def in_chunks(total, size, body):
    def step(block, _):
        body(pl.multiple_of(block * size, size))
        return 0

    lax.fori_loop(0, total // size, step, 0)


def edge_table(targets, tile):
    inside = targets[tile : tile + 1, :] - tile * TILE
    row = lax.broadcasted_iota(jnp.int32, (TILE, targets.shape[1]), 0)
    table = jnp.where(inside == row, 1.0, 0.0)
    return table.astype(jnp.bfloat16), jnp.sum(table, 1, keepdims=True)


def send_features(core, outbound, features, out, table, rows):
    table[...] = features[...].astype(jnp.float32)
    half = out.shape[0] // LANES
    first = core[0] * half

    def step(block, _):
        base = pl.multiple_of(block * 4 * half, 4 * half)
        for peer in range(4):
            for slot in range(half):
                near = outbound.at[pl.ds(peer * 2 * half + slot, outbound.shape[0] - 8 * half)]
                source = near[block * (8 * half) + first]
                rows[pl.ds(base + peer * half + slot, 1), :] = table[pl.ds(source, 1), :]
        return 0

    lax.fori_loop(0, out.shape[0] // (4 * half), step, 0)

    def narrow(base):
        out[pl.ds(base, 256), :] = rows[pl.ds(base, 256), :].astype(jnp.bfloat16)

    in_chunks(out.shape[0], 256, narrow)


def first_mix(
    live_count,
    sources,
    outbound,
    features,
    own,
    other,
    targets,
    mixed,
    words,
    table,
    picked,
    codes,
    coded_even,
    coded_odd,
):
    local = features.shape[0]
    halo = own.shape[0]
    table[0:local, :] = features[...].astype(jnp.float32)

    def widen(base):
        table[pl.ds(local + base, 256), :] = own[pl.ds(base, 256), :].astype(jnp.float32)
        table[pl.ds(local + halo + base, 256), :] = other[pl.ds(base, 256), :].astype(jnp.float32)

    in_chunks(halo, 256, widen)
    edges = targets.shape[1]
    pick_rows(sources, 0, table, picked, 0, edges * (local // TILE), 128)
    for tile in range(local // TILE):
        onehot, degree = edge_table(targets, tile)
        summed = jnp.dot(
            onehot,
            picked[tile * edges : (tile + 1) * edges, :].astype(jnp.bfloat16),
            preferred_element_type=jnp.float32,
        )
        rows = slice(tile * TILE, (tile + 1) * TILE)
        mix = (table[rows, :] + summed) / (1.0 + degree)
        mixed[rows, :] = mix
        top = jnp.maximum(jnp.max(jnp.abs(mix), 1, keepdims=True), 1e-30)
        step = jnp.clip(jnp.floor(8.0 * jnp.log2(top)) + (2.0 + SCALE_BIAS), 0.0, 255.0)
        code = jnp.round(mix * (jnp.exp2((SCALE_BIAS - step) * 0.125) * CODE_TOP))
        code = jnp.clip(code, -CODE_TOP, CODE_TOP - 1).astype(jnp.int32)
        codes[rows, :] = (code & (2**CODE_BITS - 1)) | (step.astype(jnp.int32) << CODE_BITS)

    group = lax.broadcasted_iota(jnp.int32, (8, LANES), 1) // 16

    patch = lax.broadcasted_iota(jnp.int32, (8, LANES), 0)
    count = jnp.where(patch == 0, live_count[0] & 255, live_count[0] >> 8) << 24
    patched = (lax.broadcasted_iota(jnp.int32, (8, LANES), 1) == 1) & (patch < 2)

    def pick(block, side, coded):
        for slot in range(128):
            near = outbound.at[pl.ds(side * 128 + slot, outbound.shape[0] - 255)]
            coded[slot : slot + 1, :] = codes[pl.ds(near[block * 256], 1), :]

    def pack(peer, first, coded):
        to = pl.multiple_of(peer * 40, 8)
        octet = [coded[first + 8 * k : first + 8 * k + 8, :] for k in range(8)]
        for k in range(4):
            low = (octet[k] >> 3) & 0xFFFF
            words[pl.ds(to + 8 * k, 8), :] = low | ((octet[k + 4] >> 3) << 16)
        rest = jnp.zeros((8, LANES), jnp.int32)
        steps = jnp.zeros((8, LANES), jnp.int32)
        for k in range(8):
            rest = rest | ((octet[k] & 7) << (3 * k))
            steps = jnp.where(group == k, octet[k], steps)
        rest = rest | jnp.where(patched, count, (steps >> CODE_BITS) << 24)
        words[pl.ds(to + 32, 8), :] = rest

    blocks = words.shape[0] // 160
    pick(0, 0, coded_even)

    def both(block, _):
        pick(block, 1, coded_odd)
        pack(block * 4, 0, coded_even)
        pack(block * 4 + 1, 64, coded_even)
        pick(jnp.minimum(block + 1, blocks - 1), 0, coded_even)
        pack(block * 4 + 2, 0, coded_odd)
        pack(block * 4 + 3, 64, coded_odd)
        return 0

    lax.fori_loop(0, blocks, both, 0)


def split_three(value):
    first = value.astype(jnp.bfloat16)
    rest = value - first.astype(jnp.float32)
    second = rest.astype(jnp.bfloat16)
    third = (rest - second.astype(jnp.float32)).astype(jnp.bfloat16)
    return first, second, third


def second_mix(
    core,
    live_count,
    sources,
    words,
    mixed,
    targets,
    w1_own,
    w1_other,
    b_own,
    b_other,
    w2_own,
    w2_other,
    embedded,
    sums,
    node_total,
    table,
    picked_even,
    picked_odd,
    w1,
    w2,
):
    local = mixed.shape[0]
    half = w1_own.shape[1]
    me = core[0]
    mine = pl.multiple_of(me * half, half)
    theirs = pl.multiple_of((1 - me) * half, half)
    for piece in range(3):
        w1[piece * LANES : (piece + 1) * LANES, 0:half] = w1_own[...]
        w1[piece * LANES : (piece + 1) * LANES, half : 2 * half] = w1_other[...]
    w2[0:half, 0:half] = w2_own[pl.ds(mine, half), :]
    w2[half : 2 * half, 0:half] = w2_own[pl.ds(theirs, half), :]
    w2[0:half, half : 2 * half] = w2_other[pl.ds(mine, half), :]
    w2[half : 2 * half, half : 2 * half] = w2_other[pl.ds(theirs, half), :]
    bias = jnp.concatenate([b_own[...], b_other[...]], 1)

    table[0:local, :] = mixed[...]

    def unpack(peer):
        base = pl.multiple_of(peer * 40, 8)
        to = pl.multiple_of(local + peer * 64, 64)
        pairs = [words[pl.ds(base + 8 * k, 8), :] for k in range(4)]
        rest = words[pl.ds(base + 32, 8), :]
        step = (rest >> 24) & 255
        scale = jnp.exp2((step.astype(jnp.float32) - SCALE_BIAS) * 0.125) * (1.0 / CODE_TOP)
        for k in range(8):
            high = (pairs[k] << 16) >> 16 if k < 4 else pairs[k - 4] >> 16
            code = (high << 3) | ((rest >> (3 * k)) & 7)
            table[pl.ds(to + 8 * k, 8), :] = (
                code.astype(jnp.float32) * scale[:, 16 * k : 16 * k + 1]
            )
        return step

    def unpack_several(block, counts):
        for one in range(8):
            counts = counts + unpack(block * 8 + one)
        return counts

    counts = lax.fori_loop(
        0, words.shape[0] // 320, unpack_several, jnp.zeros((8, LANES), jnp.int32)
    )
    sublane = lax.broadcasted_iota(jnp.int32, (8, LANES), 0)
    weight = jnp.where(sublane == 0, 1.0, jnp.where(sublane == 1, 256.0, 0.0))
    lane = lax.broadcasted_iota(jnp.int32, (8, LANES), 1)
    counts = jnp.where(lane == 1, counts.astype(jnp.float32) * weight, 0.0)
    counts = jnp.sum(jnp.sum(counts, 1, keepdims=True), 0, keepdims=True)
    node_total[...] = jnp.broadcast_to(counts, node_total.shape)
    edges = targets.shape[1]
    total = jnp.zeros((1, 2 * half), jnp.float32)
    squares = jnp.zeros((1, 2 * half), jnp.float32)

    def pick(tile, picked):
        picked[0:TILE, :] = mixed[tile * TILE : (tile + 1) * TILE, :]
        for edge in range(edges):
            source = sources[tile * edges + edge]
            picked[TILE + edge : TILE + edge + 1, :] = table[pl.ds(source, 1), :]

    pick(0, picked_even)
    for tile in range(local // TILE):
        rows = slice(tile * TILE, (tile + 1) * TILE)
        picked, later = (picked_even, picked_odd) if tile % 2 == 0 else (picked_odd, picked_even)
        if tile + 1 < local // TILE:
            pick(tile + 1, later)
        value = jnp.concatenate(split_three(picked[...]), 1)
        hidden = jnp.dot(value, w1[...], preferred_element_type=jnp.float32) + bias
        hidden = jnp.maximum(hidden, 0.0).astype(jnp.bfloat16)
        projected = jnp.dot(hidden, w2[...], preferred_element_type=jnp.float32)
        projected = projected.astype(jnp.bfloat16)
        onehot, degree = edge_table(targets, tile)
        summed = jnp.dot(onehot, projected[TILE:, :], preferred_element_type=jnp.float32)
        value = (projected[0:TILE, :].astype(jnp.float32) + summed) / (1.0 + degree)
        embedded[rows, :] = value
        slot = tile * TILE + lax.broadcasted_iota(jnp.int32, (TILE, 1), 0)
        value = jnp.where(slot < live_count[0], value, 0.0)
        total = total + jnp.sum(value, 0, keepdims=True)
        squares = squares + jnp.sum(value * value, 0, keepdims=True)
    for part in range(4):
        columns = slice(part * LANES, (part + 1) * LANES)
        for peer in range(sums.shape[0]):
            sums[peer, part : part + 1, :] = total[:, columns]
            sums[peer, part + 4 : part + 5, :] = squares[:, columns]


def add_and_copy(arrived, out):
    total = arrived[0]
    for peer in range(1, arrived.shape[0]):
        total = total + arrived[peer]
    for peer in range(out.shape[0]):
        out[peer] = total


def normalize(live_count, sums, node_total, embedded, out):
    total = node_total[...]
    scaled = jnp.sum(sums[...], 0) / total
    mean, square = scaled[0:4, :], scaled[4:8, :]
    dev = jnp.sqrt(square - mean * mean + 1e-05)
    slot = lax.broadcasted_iota(jnp.int32, (embedded.shape[0], 1), 0)
    live = slot < live_count[0]
    for part in range(4):
        columns = slice(part * LANES, (part + 1) * LANES)
        value = (embedded[:, columns] - mean[part : part + 1, :]) / dev[part : part + 1, :]
        out[:, columns] = jnp.where(live, value, 0.0).astype(jnp.bfloat16)


def correlate(core, own, other, normed, out):
    half = normed.shape[2]
    width = 2 * half
    groups, depth, wide = out.shape[0], out.shape[1] // 4, 4
    contract = (((0,), (0,)), ((), ()))

    def give(left, right):
        product = lax.dot_general(left, right, contract, preferred_element_type=jnp.float32)
        for group in range(groups):
            for near in range(0, depth, 2):
                rows = []
                for n1 in (near, near + 1):
                    first = ((group // wide) * depth * wide + n1 * wide + group % wide) * 4
                    rows.append(product[first : first + 4, :])
                out[group, near * 4 : near * 4 + 8, :] = jnp.concatenate(rows, 0)

    @pl.when(core[0] == 0)
    def _():
        normed[0] = own[:, 0:half]
        normed[1] = other[:, half:width]
        give(own[...], other[:, half:width])

    @pl.when(core[0] == 1)
    def _():
        normed[0] = other[:, half:width]
        normed[1] = own[:, 0:half]
        give(other[...], own[:, 0:half])


def finish(core, node, arrived, node_total, correlation, loss):
    half = correlation.shape[1]
    share, depth, wide = 4, 8, 4
    n0, n1, n2 = node[0] // (depth * wide), (node[0] // wide) % depth, node[0] % wide
    value = arrived[0]
    for peer in range(1, arrived.shape[0]):
        value = value + arrived[peer]
    value = value / node_total[0:1, 0:1]
    place = lax.broadcasted_iota(jnp.int32, value.shape, 0)
    row = ((n0 * depth + place // share) * wide + n2) * share + place % share
    column = lax.broadcasted_iota(jnp.int32, value.shape, 1) + core[0] * half
    mine = value[0:share, :]
    for other in range(1, depth):
        mine = jnp.where(n1 == other, value[other * share : (other + 1) * share, :], mine)
    correlation[...] = mine
    terms = jnp.where(row == column, jnp.square(1.0 - value), 0.005 * jnp.square(value))
    terms = jnp.sum(jnp.sum(terms, 1, keepdims=True), 0, keepdims=True)
    loss[...] = jnp.broadcast_to(terms[None], loss.shape)


def per_device(
    features, row_counts, send_rows, edge_src, edge_dst, edge_keep, w_first, b_first, w_second
):
    local, f_in = features.shape
    peers, halo = send_rows.shape[1], send_rows.shape[2]
    edges = edge_src.shape[1]
    tiles = local // TILE
    half = w_first.shape[1]
    width = 2 * half
    f32, bf16, i32 = jnp.float32, jnp.bfloat16, jnp.int32
    shape = jax.ShapeDtypeStruct
    core_index = lax.axis_index("feat")
    node_index = lax.axis_index(NODES)
    core = core_index.reshape(1).astype(i32)
    node = node_index.reshape(1).astype(i32)
    swap = [(0, 1), (1, 0)]
    planes, depth = lax.axis_size(PLANE), lax.axis_size("nodes_1")

    def partner(value):
        return lax.ppermute(value, "feat", swap)

    def sum_over_nodes(blocks, name):
        blocks = lax.all_to_all(blocks, PLANE, split_axis=0, concat_axis=0, tiled=True)
        copies = call(
            add_and_copy, shape((depth, *blocks.shape[1:]), f32), [], blocks, name=name
        )
        return lax.all_to_all(copies, "nodes_1", split_axis=0, concat_axis=0, tiled=True)

    w1_other, w2_other = partner(w_first), partner(w_second)
    bias = b_first.reshape(1, half)
    bias_other = partner(bias)
    outbound = send_rows.reshape(peers * halo)
    sources = lax.dynamic_index_in_dim(edge_src, core_index, 0, False)
    targets = lax.dynamic_index_in_dim(edge_dst, core_index, 0, False)
    kept = lax.dynamic_index_in_dim(edge_keep, core_index, 0, False)
    targets = jnp.where(kept == 1, targets, -1).reshape(tiles, edges // tiles)

    rows_half = peers * halo // 2
    sent = call(
        send_features,
        shape((rows_half, f_in), bf16),
        [pltpu.VMEM((local, f_in), f32), pltpu.VMEM((rows_half, f_in), f32)],
        features,
        scalars=(core, outbound),
        name="send_features",
    )
    sent, w1_other, w2_other, bias_other = lax.optimization_barrier(
        (sent, w1_other, w2_other, bias_other)
    )
    got = lax.all_to_all(
        sent.reshape(peers, halo // 2, f_in), NODES, split_axis=0, concat_axis=0, tiled=True
    )
    got_other = partner(got)
    remote = sources - local
    slot_half = (remote % halo) // (halo // 2)
    from_other = (slot_half != core_index).astype(i32)
    remote = (remote // halo) * (halo // 2) + remote % (halo // 2) + from_other * rows_half
    first_sources = jnp.where(sources < local, sources, remote + local)
    mixed, words = call(
        first_mix,
        (shape((local, f_in), f32), shape((peers * 40, f_in), i32)),
        [
            pltpu.VMEM((local + 2 * rows_half, f_in), f32),
            pltpu.VMEM((edges, f_in), f32),
            pltpu.VMEM((local, f_in), i32),
            pltpu.VMEM((2 * halo, f_in), i32),
            pltpu.VMEM((2 * halo, f_in), i32),
        ],
        features,
        got.reshape(rows_half, f_in),
        got_other.reshape(rows_half, f_in),
        targets,
        scalars=(row_counts, first_sources, outbound),
        name="first_mix",
    )
    arrived = lax.all_to_all(
        words.reshape(peers, 40, f_in), NODES, split_axis=0, concat_axis=0, tiled=True
    )
    embedded, sums, node_total = call(
        second_mix,
        (
            shape((local, width), f32),
            shape((planes, 8, LANES), f32),
            shape((8, LANES), f32),
        ),
        [
            pltpu.VMEM((local + peers * halo, f_in), f32),
            pltpu.VMEM((TILE + edges // tiles, f_in), f32),
            pltpu.VMEM((TILE + edges // tiles, f_in), f32),
            pltpu.VMEM((3 * f_in, width), bf16),
            pltpu.VMEM((width, width), bf16),
        ],
        arrived.reshape(peers * 40, f_in),
        mixed,
        targets,
        w_first,
        w1_other,
        bias,
        bias_other,
        w_second,
        w2_other,
        scalars=(core, row_counts, sources),
        name="second_mix",
    )
    sums = sum_over_nodes(sums, "add_sums")
    own = call(
        normalize,
        shape((local, width), bf16),
        [],
        sums,
        node_total,
        embedded,
        scalars=(row_counts,),
        name="normalize",
    )
    normed, partial = call(
        correlate,
        (shape((2, local, half), bf16), shape((planes, width // planes, half), f32)),
        [],
        own,
        partner(own),
        scalars=(core,),
        name="correlate",
    )
    partial = sum_over_nodes(partial, "add_products")
    devices = lax.axis_size(PLANE_FEAT)
    correlation, loss = call(
        finish,
        (shape((width // peers, half), f32), shape((devices, 1, LANES), f32)),
        [],
        partial,
        node_total,
        scalars=(core, node),
        name="finish",
    )
    losses = lax.all_to_all(loss, PLANE_FEAT, 0, 0, tiled=True)
    return (normed, correlation, jnp.sum(losses[:, 0, 0]))


def solution(mesh):
    torus = Mesh(
        mesh.devices.reshape(4, 8, 4, mesh.shape["feat"]), ("nodes_0", "nodes_1", "nodes_2", "feat")
    )
    placed = (
        P(NODES, None),
        P(NODES),
        P(NODES, None, None),
        P(None, NODES),
        P(None, NODES),
        P(None, NODES),
        P(None, "feat"),
        P("feat"),
        P(None, "feat"),
    )
    return jax.shard_map(
        per_device,
        mesh=torus,
        in_specs=placed,
        out_specs=(P(None, NODES, "feat"), P(NODES, "feat"), P()),
        check_vma=False,
    )
```

```python
import functools

import jax
import jax.numpy as jnp
from jax import lax
from jax.experimental import pallas as pl
from jax.experimental.pallas import tpu as pltpu
from jax.sharding import Mesh
from jax.sharding import PartitionSpec as P

NODES = ("nodes_0", "nodes_1", "nodes_2")
PLANE = ("nodes_0", "nodes_2")
PLANE_FEAT = ("nodes_0", "nodes_2", "feat")

LANES = 128
TILE = 128
CODE_BITS = 18
CODE_TOP = 2 ** (CODE_BITS - 1)
SCALE_BIAS = 224.0
COARSE = 5
PACKED = 36

VMEM = pl.BlockSpec(memory_space=pltpu.VMEM)
SMEM = pl.BlockSpec(memory_space=pltpu.SMEM)


def call(body, outs, scratch, *operands, scalars=(), name):
    return pl.pallas_call(
        body,
        out_shape=outs,
        in_specs=[SMEM] * len(scalars) + [VMEM] * len(operands),
        out_specs=jax.tree.map(lambda _: VMEM, outs),
        scratch_shapes=scratch,
        compiler_params=pltpu.CompilerParams(vmem_limit_bytes=26 * 2**20),
        name=name,
    )(*scalars, *operands)


def pick_rows(index, first_index, table, rows, first_row, count, unroll):
    def step(block, _):
        base = pl.multiple_of(block * unroll, unroll)
        for lane in range(unroll):
            source = index.at[pl.ds(lane, index.shape[0] - unroll)][first_index + base]
            rows[pl.ds(first_row + base + lane, 1), :] = table[pl.ds(source, 1), :]
        return 0

    lax.fori_loop(0, count // unroll, step, 0)


def in_chunks(total, size, body):
    def step(block, _):
        body(pl.multiple_of(block * size, size))
        return 0

    lax.fori_loop(0, total // size, step, 0)


def edge_table(targets, tile):
    inside = targets[tile : tile + 1, :] - tile * TILE
    row = lax.broadcasted_iota(jnp.int32, (TILE, targets.shape[1]), 0)
    table = jnp.where(inside == row, 1.0, 0.0)
    return table.astype(jnp.bfloat16), jnp.sum(table, 1, keepdims=True)


def send_features(core, outbound, features, out, table, rows):
    table[...] = features[...].astype(jnp.float32)
    half = out.shape[0] // LANES
    first = core[0] * half

    def step(block, _):
        base = pl.multiple_of(block * 4 * half, 4 * half)
        for peer in range(4):
            for slot in range(half):
                near = outbound.at[pl.ds(peer * 2 * half + slot, outbound.shape[0] - 8 * half)]
                source = near[block * (8 * half) + first]
                rows[pl.ds(base + peer * half + slot, 1), :] = table[pl.ds(source, 1), :]
        return 0

    lax.fori_loop(0, out.shape[0] // (4 * half), step, 0)

    def narrow(base):
        out[pl.ds(base, 256), :] = rows[pl.ds(base, 256), :].astype(jnp.bfloat16)

    in_chunks(out.shape[0], 256, narrow)


def first_mix(
    live_count,
    sources,
    outbound,
    features,
    own,
    other,
    targets,
    mixed,
    words,
    table,
    picked,
    codes,
    coded_even,
    coded_odd,
):
    local = features.shape[0]
    halo = own.shape[0]
    table[0:local, :] = features[...]

    def widen(base):
        table[pl.ds(local + base, 256), :] = own[pl.ds(base, 256), :].astype(jnp.float32)
        table[pl.ds(local + halo + base, 256), :] = other[pl.ds(base, 256), :].astype(jnp.float32)

    in_chunks(halo, 256, widen)
    edges = targets.shape[1]
    pick_rows(sources, 0, table, picked, 0, edges * (local // TILE), 128)
    for tile in range(local // TILE):
        onehot, degree = edge_table(targets, tile)
        summed = jnp.dot(
            onehot,
            picked[tile * edges : (tile + 1) * edges, :].astype(jnp.bfloat16),
            preferred_element_type=jnp.float32,
        )
        rows = slice(tile * TILE, (tile + 1) * TILE)
        mix = (table[rows, :] + summed) / (1.0 + degree)
        mixed[rows, :] = mix
        top = jnp.maximum(jnp.max(jnp.abs(mix), 1, keepdims=True), 1e-30)
        step = jnp.clip(jnp.floor(8.0 * jnp.log2(top)) + (2.0 + SCALE_BIAS), 0.0, 255.0)
        code = jnp.round(mix * (jnp.exp2((SCALE_BIAS - step) * 0.125) * CODE_TOP))
        code = jnp.clip(code, -CODE_TOP, CODE_TOP - 1).astype(jnp.int32)
        codes[rows, :] = (code & (2**CODE_BITS - 1)) | (step.astype(jnp.int32) << CODE_BITS)

    lane = lax.broadcasted_iota(jnp.int32, (8, LANES), 1)
    row = lax.broadcasted_iota(jnp.int32, (8, LANES), 0)
    counted = jnp.where((lane == COARSE - 1) & (row == 0), live_count[0], 0)

    def pick(block, side, coded):
        for slot in range(128):
            near = outbound.at[pl.ds(side * 128 + slot, outbound.shape[0] - 255)]
            coded[slot : slot + 1, :] = codes[pl.ds(near[block * 256], 1), :]

    def pack(peer, first, coded):
        to = peer * PACKED
        octet = [coded[first + 8 * k : first + 8 * k + 8, :] for k in range(8)]
        for k in range(4):
            low = (octet[k] >> 2) & 0xFFFF
            words[pl.ds(to + 8 * k, 8), :] = low | ((octet[k + 4] >> 2) << 16)
        fine = jnp.zeros((8, LANES), jnp.int32)
        coarse = counted
        for k in range(8):
            fine = fine | ((octet[k] & 3) << (4 * k + 2 * (row // 4)))
            scale = (octet[k] >> CODE_BITS) << (16 * (k % 2) + 8 * (row // 4))
            coarse = coarse | jnp.where(lane == k // 2, scale, 0)
        fine = jnp.where(lane < COARSE, coarse, fine)
        words[pl.ds(to + 32, 4), :] = fine[0:4, :] | fine[4:8, :]

    blocks = words.shape[0] // (4 * PACKED)
    pick(0, 0, coded_even)

    def both(block, _):
        pick(block, 1, coded_odd)
        pack(block * 4, 0, coded_even)
        pack(block * 4 + 1, 64, coded_even)
        pick(jnp.minimum(block + 1, blocks - 1), 0, coded_even)
        pack(block * 4 + 2, 0, coded_odd)
        pack(block * 4 + 3, 64, coded_odd)
        return 0

    lax.fori_loop(0, blocks, both, 0)


def split_three(value):
    first = value.astype(jnp.bfloat16)
    rest = value - first.astype(jnp.float32)
    second = rest.astype(jnp.bfloat16)
    third = (rest - second.astype(jnp.float32)).astype(jnp.bfloat16)
    return first, second, third


def second_mix(
    core,
    live_count,
    sources,
    words,
    mixed,
    targets,
    w1_own,
    w1_other,
    b_own,
    b_other,
    w2_own,
    w2_other,
    embedded,
    sums,
    node_total,
    table,
    picked_even,
    picked_odd,
    w1,
    w2,
):
    local = mixed.shape[0]
    half = w1_own.shape[1]
    me = core[0]
    mine = pl.multiple_of(me * half, half)
    theirs = pl.multiple_of((1 - me) * half, half)
    for piece in range(3):
        w1[piece * LANES : (piece + 1) * LANES, 0:half] = w1_own[...]
        w1[piece * LANES : (piece + 1) * LANES, half : 2 * half] = w1_other[...]
    w2[0:half, 0:half] = w2_own[pl.ds(mine, half), :]
    w2[half : 2 * half, 0:half] = w2_own[pl.ds(theirs, half), :]
    w2[0:half, half : 2 * half] = w2_other[pl.ds(mine, half), :]
    w2[half : 2 * half, half : 2 * half] = w2_other[pl.ds(theirs, half), :]
    bias = jnp.concatenate([b_own[...], b_other[...]], 1)

    table[0:local, :] = mixed[...]

    lane = lax.broadcasted_iota(jnp.int32, (8, LANES), 1)
    row = lax.broadcasted_iota(jnp.int32, (8, LANES), 0)

    def unpack(peer):
        base = peer * PACKED
        to = pl.multiple_of(local + peer * 64, 64)
        pairs = [words[pl.ds(base + 8 * k, 8), :] for k in range(4)]
        rest = words[pl.ds(base + 28, 8), :]
        rest = jnp.where(row < 4, pltpu.roll(rest, 4, 0), rest)
        scales = []
        for side in range(2):
            step = (rest >> (16 * side + 8 * (row // 4))) & 255
            scale = jnp.exp2((step.astype(jnp.float32) - SCALE_BIAS) * 0.125)
            scales.append(scale * (1.0 / CODE_TOP))
        fine = jnp.where(lane < COARSE, -0x55555556, rest)
        for k in range(8):
            high = (pairs[k] << 16) >> 16 if k < 4 else pairs[k - 4] >> 16
            code = (high << 2) | ((fine >> (4 * k + 2 * (row // 4))) & 3)
            scale = scales[k % 2][:, k // 2 : k // 2 + 1]
            table[pl.ds(to + 8 * k, 8), :] = code.astype(jnp.float32) * scale
        return rest

    def unpack_several(block, counts):
        for one in range(8):
            counts = counts + unpack(block * 8 + one)
        return counts

    counts = lax.fori_loop(
        0, words.shape[0] // (8 * PACKED), unpack_several, jnp.zeros((8, LANES), jnp.int32)
    )
    counts = jnp.where((lane == COARSE - 1) & (row == 0), counts, 0).astype(jnp.float32)
    counts = jnp.sum(jnp.sum(counts, 1, keepdims=True), 0, keepdims=True)
    node_total[...] = jnp.broadcast_to(counts, node_total.shape)
    edges = targets.shape[1]
    total = jnp.zeros((1, 2 * half), jnp.float32)
    squares = jnp.zeros((1, 2 * half), jnp.float32)

    def pick(tile, picked):
        picked[0:TILE, :] = mixed[tile * TILE : (tile + 1) * TILE, :]
        for edge in range(edges):
            source = sources[tile * edges + edge]
            picked[TILE + edge : TILE + edge + 1, :] = table[pl.ds(source, 1), :]

    pick(0, picked_even)
    for tile in range(local // TILE):
        rows = slice(tile * TILE, (tile + 1) * TILE)
        picked, later = (picked_even, picked_odd) if tile % 2 == 0 else (picked_odd, picked_even)
        if tile + 1 < local // TILE:
            pick(tile + 1, later)
        value = jnp.concatenate(split_three(picked[...]), 1)
        hidden = jnp.dot(value, w1[...], preferred_element_type=jnp.float32) + bias
        hidden = jnp.maximum(hidden, 0.0).astype(jnp.bfloat16)
        projected = jnp.dot(hidden, w2[...], preferred_element_type=jnp.float32)
        projected = projected.astype(jnp.bfloat16)
        onehot, degree = edge_table(targets, tile)
        summed = jnp.dot(onehot, projected[TILE:, :], preferred_element_type=jnp.float32)
        value = (projected[0:TILE, :].astype(jnp.float32) + summed) / (1.0 + degree)
        embedded[rows, :] = value
        slot = tile * TILE + lax.broadcasted_iota(jnp.int32, (TILE, 1), 0)
        value = jnp.where(slot < live_count[0], value, 0.0)
        total = total + jnp.sum(value, 0, keepdims=True)
        squares = squares + jnp.sum(value * value, 0, keepdims=True)
    for part in range(4):
        columns = slice(part * LANES, (part + 1) * LANES)
        for peer in range(sums.shape[0]):
            sums[peer, part : part + 1, :] = total[:, columns]
            sums[peer, part + 4 : part + 5, :] = squares[:, columns]


def add_and_copy(arrived, out):
    total = arrived[0]
    for peer in range(1, arrived.shape[0]):
        total = total + arrived[peer]
    for peer in range(out.shape[0]):
        out[peer] = total


def normalize(live_count, sums, node_total, embedded, out):
    total = node_total[...]
    scaled = jnp.sum(sums[...], 0) / total
    mean, square = scaled[0:4, :], scaled[4:8, :]
    dev = jnp.sqrt(square - mean * mean + 1e-05)
    slot = lax.broadcasted_iota(jnp.int32, (embedded.shape[0], 1), 0)
    live = slot < live_count[0]
    for part in range(4):
        columns = slice(part * LANES, (part + 1) * LANES)
        value = (embedded[:, columns] - mean[part : part + 1, :]) / dev[part : part + 1, :]
        out[:, columns] = jnp.where(live, value, 0.0).astype(jnp.bfloat16)


def correlate(core, own, other, normed, out):
    half = normed.shape[2]
    width = 2 * half
    groups, depth, wide = out.shape[0], out.shape[1] // 4, 4
    contract = (((0,), (0,)), ((), ()))

    def give(left, right):
        product = lax.dot_general(left, right, contract, preferred_element_type=jnp.float32)
        for group in range(groups):
            for near in range(0, depth, 2):
                rows = []
                for n1 in (near, near + 1):
                    first = ((group // wide) * depth * wide + n1 * wide + group % wide) * 4
                    rows.append(product[first : first + 4, :])
                out[group, near * 4 : near * 4 + 8, :] = jnp.concatenate(rows, 0)

    @pl.when(core[0] == 0)
    def _():
        normed[0] = own[:, 0:half]
        normed[1] = other[:, half:width]
        give(own[...], other[:, half:width])

    @pl.when(core[0] == 1)
    def _():
        normed[0] = other[:, half:width]
        normed[1] = own[:, 0:half]
        give(other[...], own[:, 0:half])


def finish(core, node, arrived, node_total, correlation, loss):
    half = correlation.shape[1]
    share, depth, wide = 4, 8, 4
    n0, n1, n2 = node[0] // (depth * wide), (node[0] // wide) % depth, node[0] % wide
    value = arrived[0]
    for peer in range(1, arrived.shape[0]):
        value = value + arrived[peer]
    value = value / node_total[0:1, 0:1]
    place = lax.broadcasted_iota(jnp.int32, value.shape, 0)
    row = ((n0 * depth + place // share) * wide + n2) * share + place % share
    column = lax.broadcasted_iota(jnp.int32, value.shape, 1) + core[0] * half
    mine = value[0:share, :]
    for other in range(1, depth):
        mine = jnp.where(n1 == other, value[other * share : (other + 1) * share, :], mine)
    correlation[...] = mine
    terms = jnp.where(row == column, jnp.square(1.0 - value), 0.005 * jnp.square(value))
    terms = jnp.sum(jnp.sum(terms, 1, keepdims=True), 0, keepdims=True)
    loss[...] = jnp.broadcast_to(terms[None], loss.shape)


def per_device(
    features, row_counts, send_rows, edge_src, edge_dst, edge_keep, w_first, b_first, w_second
):
    local, f_in = features.shape
    peers, halo = send_rows.shape[1], send_rows.shape[2]
    edges = edge_src.shape[1]
    tiles = local // TILE
    half = w_first.shape[1]
    width = 2 * half
    f32, bf16, i32 = jnp.float32, jnp.bfloat16, jnp.int32
    shape = jax.ShapeDtypeStruct
    core_index = lax.axis_index("feat")
    node_index = lax.axis_index(NODES)
    core = core_index.reshape(1).astype(i32)
    node = node_index.reshape(1).astype(i32)
    swap = [(0, 1), (1, 0)]
    planes, depth = lax.axis_size(PLANE), lax.axis_size("nodes_1")

    def partner(value):
        return lax.ppermute(value, "feat", swap)

    def sum_over_nodes(blocks, name):
        blocks = lax.all_to_all(blocks, PLANE, split_axis=0, concat_axis=0, tiled=True)
        copies = call(
            add_and_copy, shape((depth, *blocks.shape[1:]), f32), [], blocks, name=name
        )
        return lax.all_to_all(copies, "nodes_1", split_axis=0, concat_axis=0, tiled=True)

    w1_other, w2_other = partner(w_first), partner(w_second)
    bias = b_first.reshape(1, half)
    bias_other = partner(bias)
    outbound = send_rows.reshape(peers * halo)
    sources = lax.dynamic_index_in_dim(edge_src, core_index, 0, False)
    targets = lax.dynamic_index_in_dim(edge_dst, core_index, 0, False)
    kept = lax.dynamic_index_in_dim(edge_keep, core_index, 0, False)
    targets = jnp.where(kept == 1, targets, -1).reshape(tiles, edges // tiles)

    rows_half = peers * halo // 2
    sent, wide = call(
        send_features,
        (shape((rows_half, f_in), bf16), shape((local, f_in), f32)),
        [pltpu.VMEM((rows_half, f_in), f32)],
        features,
        scalars=(core, outbound),
        name="send_features",
    )
    sent, w1_other, w2_other, bias_other = lax.optimization_barrier(
        (sent, w1_other, w2_other, bias_other)
    )
    got = lax.all_to_all(
        sent.reshape(peers, halo // 2, f_in), NODES, split_axis=0, concat_axis=0, tiled=True
    )
    got_other = partner(got)
    remote = sources - local
    slot_half = (remote % halo) // (halo // 2)
    from_other = (slot_half != core_index).astype(i32)
    remote = (remote // halo) * (halo // 2) + remote % (halo // 2) + from_other * rows_half
    first_sources = jnp.where(sources < local, sources, remote + local)
    mixed, words = call(
        first_mix,
        (shape((local, f_in), f32), shape((peers * PACKED, f_in), i32)),
        [
            pltpu.VMEM((local + 2 * rows_half, f_in), f32),
            pltpu.VMEM((edges, f_in), f32),
            pltpu.VMEM((local, f_in), i32),
            pltpu.VMEM((2 * halo, f_in), i32),
            pltpu.VMEM((2 * halo, f_in), i32),
        ],
        wide,
        got.reshape(rows_half, f_in),
        got_other.reshape(rows_half, f_in),
        targets,
        scalars=(row_counts, first_sources, outbound),
        name="first_mix",
    )
    arrived = lax.all_to_all(
        words.reshape(peers * PACKED // 4, 4, f_in), NODES, split_axis=0, concat_axis=0, tiled=True
    )
    embedded, sums, node_total = call(
        second_mix,
        (
            shape((local, width), f32),
            shape((planes, 8, LANES), f32),
            shape((8, LANES), f32),
        ),
        [
            pltpu.VMEM((local + peers * halo, f_in), f32),
            pltpu.VMEM((TILE + edges // tiles, f_in), f32),
            pltpu.VMEM((TILE + edges // tiles, f_in), f32),
            pltpu.VMEM((3 * f_in, width), bf16),
            pltpu.VMEM((width, width), bf16),
        ],
        arrived.reshape(peers * PACKED, f_in),
        mixed,
        targets,
        w_first,
        w1_other,
        bias,
        bias_other,
        w_second,
        w2_other,
        scalars=(core, row_counts, sources),
        name="second_mix",
    )
    sums = sum_over_nodes(sums, "add_sums")
    own = call(
        normalize,
        shape((local, width), bf16),
        [],
        sums,
        node_total,
        embedded,
        scalars=(row_counts,),
        name="normalize",
    )
    normed, partial = call(
        correlate,
        (shape((2, local, half), bf16), shape((planes, width // planes, half), f32)),
        [],
        own,
        partner(own),
        scalars=(core,),
        name="correlate",
    )
    partial = sum_over_nodes(partial, "add_products")
    devices = lax.axis_size(PLANE_FEAT)
    correlation, loss = call(
        finish,
        (shape((width // peers, half), f32), shape((devices, 1, LANES), f32)),
        [],
        partial,
        node_total,
        scalars=(core, node),
        name="finish",
    )
    losses = lax.all_to_all(loss, PLANE_FEAT, 0, 0, tiled=True)
    return (normed, correlation, jnp.sum(losses[:, 0, 0]))


def solution(mesh):
    torus = Mesh(
        mesh.devices.reshape(4, 8, 4, mesh.shape["feat"]), ("nodes_0", "nodes_1", "nodes_2", "feat")
    )
    placed = (
        P(NODES, None),
        P(NODES),
        P(NODES, None, None),
        P(None, NODES),
        P(None, NODES),
        P(None, NODES),
        P(None, "feat"),
        P("feat"),
        P(None, "feat"),
    )
    return jax.shard_map(
        per_device,
        mesh=torus,
        in_specs=placed,
        out_specs=(P(None, NODES, "feat"), P(NODES, "feat"), P()),
        check_vma=False,
    )
```

```python
import functools

import jax
import jax.numpy as jnp
from jax import lax
from jax.experimental import pallas as pl
from jax.experimental.pallas import tpu as pltpu
from jax.sharding import Mesh
from jax.sharding import PartitionSpec as P

NODES = ("nodes_0", "nodes_1", "nodes_2")
PLANE = ("nodes_0", "nodes_2")
PLANE_FEAT = ("nodes_0", "nodes_2", "feat")
NODES_FEAT = ("nodes_0", "nodes_1", "nodes_2", "feat")

LANES = 128
TILE = 128
CODE_BITS = 18
CODE_TOP = 2 ** (CODE_BITS - 1)
SCALE_BIAS = 224.0
COARSE = 5
PACKED = 36

VMEM = pl.BlockSpec(memory_space=pltpu.VMEM)
SMEM = pl.BlockSpec(memory_space=pltpu.SMEM)


def call(body, outs, scratch, *operands, scalars=(), name):
    return pl.pallas_call(
        body,
        out_shape=outs,
        in_specs=[SMEM] * len(scalars) + [VMEM] * len(operands),
        out_specs=jax.tree.map(lambda _: VMEM, outs),
        scratch_shapes=scratch,
        compiler_params=pltpu.CompilerParams(vmem_limit_bytes=26 * 2**20),
        name=name,
    )(*scalars, *operands)


def in_chunks(total, size, body):
    def step(block, _):
        body(pl.multiple_of(block * size, size))
        return 0

    lax.fori_loop(0, total // size, step, 0)


def edge_table(targets, tile):
    inside = targets[tile : tile + 1, :] - tile * TILE
    row = lax.broadcasted_iota(jnp.int32, (TILE, targets.shape[1]), 0)
    table = jnp.where(inside == row, 1.0, 0.0)
    return table.astype(jnp.bfloat16), jnp.sum(table, 1, keepdims=True)


def place_of(core, peer, peers):
    return jnp.where(core[0] == 0, peer, peers - 1 - peer)


def send_features(core, outbound, features, out, table, rows):
    table[...] = features[...].astype(jnp.float32)
    half = out.shape[0] // LANES
    first = core[0] * half

    def step(block, _):
        place = place_of(core, block, out.shape[0] // (4 * half))
        base = pl.multiple_of(place * 4 * half, 4 * half)
        for peer in range(4):
            to = base + jnp.where(core[0] == 0, peer, 3 - peer) * half
            for slot in range(half):
                near = outbound.at[pl.ds(peer * 2 * half + slot, outbound.shape[0] - 8 * half)]
                source = near[block * (8 * half) + first]
                rows[pl.ds(to + slot, 1), :] = table[pl.ds(source, 1), :]
        return 0

    lax.fori_loop(0, out.shape[0] // (4 * half), step, 0)

    def narrow(base):
        out[pl.ds(base, 256), :] = rows[pl.ds(base, 256), :].astype(jnp.bfloat16)

    in_chunks(out.shape[0], 256, narrow)


def first_mix(
    core,
    live_count,
    sources,
    outbound,
    features,
    own,
    other,
    targets,
    mixed,
    words,
    table,
    picked_even,
    picked_odd,
    codes,
    coded_even,
    coded_odd,
):
    local = features.shape[0]
    halo = own.shape[0]
    table[0:local, :] = features[...]

    def widen(base):
        table[pl.ds(local + base, 256), :] = own[pl.ds(base, 256), :].astype(jnp.float32)
        table[pl.ds(local + halo + base, 256), :] = other[pl.ds(base, 256), :].astype(jnp.float32)

    in_chunks(halo, 256, widen)
    edges = targets.shape[1]

    def pick(tile, picked):
        for edge in range(edges):
            source = sources[tile * edges + edge]
            picked[edge : edge + 1, :] = table[pl.ds(source, 1), :]

    pick(0, picked_even)
    for tile in range(local // TILE):
        picked, later = (picked_even, picked_odd) if tile % 2 == 0 else (picked_odd, picked_even)
        if tile + 1 < local // TILE:
            pick(tile + 1, later)
        onehot, degree = edge_table(targets, tile)
        summed = jnp.dot(
            onehot, picked[...].astype(jnp.bfloat16), preferred_element_type=jnp.float32
        )
        rows = slice(tile * TILE, (tile + 1) * TILE)
        mix = (table[rows, :] + summed) / (1.0 + degree)
        mixed[rows, :] = mix
        top = jnp.maximum(jnp.max(jnp.abs(mix), 1, keepdims=True), 1e-30)
        step = jnp.clip(jnp.floor(8.0 * jnp.log2(top)) + (2.0 + SCALE_BIAS), 0.0, 255.0)
        code = jnp.round(mix * (jnp.exp2((SCALE_BIAS - step) * 0.125) * CODE_TOP))
        code = jnp.clip(code, -CODE_TOP, CODE_TOP - 1).astype(jnp.int32)
        codes[rows, :] = (code & (2**CODE_BITS - 1)) | (step.astype(jnp.int32) << CODE_BITS)

    lane = lax.broadcasted_iota(jnp.int32, (8, LANES), 1)
    row = lax.broadcasted_iota(jnp.int32, (8, LANES), 0)
    counted = jnp.where((lane == COARSE - 1) & (row == 0), live_count[0], 0)

    def pick_slots(block, side, coded):
        for slot in range(128):
            near = outbound.at[pl.ds(side * 128 + slot, outbound.shape[0] - 255)]
            coded[slot : slot + 1, :] = codes[pl.ds(near[block * 256], 1), :]

    def pack(peer, first, coded):
        to = place_of(core, peer, words.shape[0] // PACKED) * PACKED
        octet = [coded[first + 8 * k : first + 8 * k + 8, :] for k in range(8)]
        for k in range(4):
            low = (octet[k] >> 2) & 0xFFFF
            words[pl.ds(to + 8 * k, 8), :] = low | ((octet[k + 4] >> 2) << 16)
        fine = jnp.zeros((8, LANES), jnp.int32)
        coarse = counted
        for k in range(8):
            fine = fine | ((octet[k] & 3) << (4 * k + 2 * (row // 4)))
            scale = (octet[k] >> CODE_BITS) << (16 * (k % 2) + 8 * (row // 4))
            coarse = coarse | jnp.where(lane == k // 2, scale, 0)
        fine = jnp.where(lane < COARSE, coarse, fine)
        words[pl.ds(to + 32, 4), :] = fine[0:4, :] | fine[4:8, :]

    blocks = words.shape[0] // (4 * PACKED)
    pick_slots(0, 0, coded_even)

    def both(block, _):
        pick_slots(block, 1, coded_odd)
        pack(block * 4, 0, coded_even)
        pack(block * 4 + 1, 64, coded_even)
        pick_slots(jnp.minimum(block + 1, blocks - 1), 0, coded_even)
        pack(block * 4 + 2, 0, coded_odd)
        pack(block * 4 + 3, 64, coded_odd)
        return 0

    lax.fori_loop(0, blocks, both, 0)


def split_three(value):
    first = value.astype(jnp.bfloat16)
    rest = value - first.astype(jnp.float32)
    second = rest.astype(jnp.bfloat16)
    third = (rest - second.astype(jnp.float32)).astype(jnp.bfloat16)
    return first, second, third


def second_mix(
    core,
    live_count,
    sources,
    words,
    mixed,
    targets,
    w1_own,
    w1_other,
    b_own,
    b_other,
    w2_own,
    w2_other,
    embedded,
    sums,
    node_total,
    table,
    picked_even,
    picked_odd,
    w1,
    w2,
):
    local = mixed.shape[0]
    half = w1_own.shape[1]
    me = core[0]
    mine = pl.multiple_of(me * half, half)
    theirs = pl.multiple_of((1 - me) * half, half)
    for piece in range(3):
        w1[piece * LANES : (piece + 1) * LANES, 0:half] = w1_own[...]
        w1[piece * LANES : (piece + 1) * LANES, half : 2 * half] = w1_other[...]
    w2[0:half, 0:half] = w2_own[pl.ds(mine, half), :]
    w2[half : 2 * half, 0:half] = w2_own[pl.ds(theirs, half), :]
    w2[0:half, half : 2 * half] = w2_other[pl.ds(mine, half), :]
    w2[half : 2 * half, half : 2 * half] = w2_other[pl.ds(theirs, half), :]
    bias = jnp.concatenate([b_own[...], b_other[...]], 1)

    table[0:local, :] = mixed[...]

    lane = lax.broadcasted_iota(jnp.int32, (8, LANES), 1)
    row = lax.broadcasted_iota(jnp.int32, (8, LANES), 0)

    def unpack(peer):
        base = peer * PACKED
        to = place_of(core, peer, words.shape[0] // PACKED) * 64
        to = pl.multiple_of(local + to, 64)
        pairs = [words[pl.ds(base + 8 * k, 8), :] for k in range(4)]
        rest = words[pl.ds(base + 28, 8), :]
        rest = jnp.where(row < 4, pltpu.roll(rest, 4, 0), rest)
        scales = []
        for side in range(2):
            step = (rest >> (16 * side + 8 * (row // 4))) & 255
            scale = jnp.exp2((step.astype(jnp.float32) - SCALE_BIAS) * 0.125)
            scales.append(scale * (1.0 / CODE_TOP))
        fine = jnp.where(lane < COARSE, -0x55555556, rest)
        for k in range(8):
            high = (pairs[k] << 16) >> 16 if k < 4 else pairs[k - 4] >> 16
            code = (high << 2) | ((fine >> (4 * k + 2 * (row // 4))) & 3)
            scale = scales[k % 2][:, k // 2 : k // 2 + 1]
            table[pl.ds(to + 8 * k, 8), :] = code.astype(jnp.float32) * scale
        return rest

    def unpack_several(block, counts):
        for one in range(8):
            counts = counts + unpack(block * 8 + one)
        return counts

    counts = lax.fori_loop(
        0, words.shape[0] // (8 * PACKED), unpack_several, jnp.zeros((8, LANES), jnp.int32)
    )
    counts = jnp.where((lane == COARSE - 1) & (row == 0), counts, 0).astype(jnp.float32)
    counts = jnp.sum(jnp.sum(counts, 1, keepdims=True), 0, keepdims=True)
    node_total[...] = jnp.broadcast_to(counts, node_total.shape)
    edges = targets.shape[1]
    total = jnp.zeros((1, 2 * half), jnp.float32)
    squares = jnp.zeros((1, 2 * half), jnp.float32)

    def pick(tile, picked):
        picked[0:TILE, :] = mixed[tile * TILE : (tile + 1) * TILE, :]
        for edge in range(edges):
            source = sources[tile * edges + edge]
            picked[TILE + edge : TILE + edge + 1, :] = table[pl.ds(source, 1), :]

    pick(0, picked_even)
    for tile in range(local // TILE):
        rows = slice(tile * TILE, (tile + 1) * TILE)
        picked, later = (picked_even, picked_odd) if tile % 2 == 0 else (picked_odd, picked_even)
        if tile + 1 < local // TILE:
            pick(tile + 1, later)
        value = jnp.concatenate(split_three(picked[...]), 1)
        hidden = jnp.dot(value, w1[...], preferred_element_type=jnp.float32) + bias
        hidden = jnp.maximum(hidden, 0.0).astype(jnp.bfloat16)
        projected = jnp.dot(hidden, w2[...], preferred_element_type=jnp.float32)
        projected = projected.astype(jnp.bfloat16)
        onehot, degree = edge_table(targets, tile)
        summed = jnp.dot(onehot, projected[TILE:, :], preferred_element_type=jnp.float32)
        value = (projected[0:TILE, :].astype(jnp.float32) + summed) / (1.0 + degree)
        embedded[rows, :] = value
        slot = tile * TILE + lax.broadcasted_iota(jnp.int32, (TILE, 1), 0)
        value = jnp.where(slot < live_count[0], value, 0.0)
        total = total + jnp.sum(value, 0, keepdims=True)
        squares = squares + jnp.sum(value * value, 0, keepdims=True)
    for part in range(4):
        columns = slice(part * LANES, (part + 1) * LANES)
        for peer in range(sums.shape[0]):
            sums[peer, part : part + 1, :] = total[:, columns]
            sums[peer, part + 4 : part + 5, :] = squares[:, columns]


def add_and_copy(arrived, out):
    total = arrived[0]
    for peer in range(1, arrived.shape[0]):
        total = total + arrived[peer]
    for peer in range(out.shape[0]):
        out[peer] = total


def put_products(out, place, values):
    sides = [[values[8 * m : 8 * m + 8, side : side + LANES] for side in (0, LANES)] for m in range(4)]
    top = jnp.zeros((8, LANES), jnp.float32)
    for pair in sides:
        for side in pair:
            top = jnp.maximum(top, jnp.abs(side))
    top = jnp.maximum(jnp.max(top, 0, keepdims=True), 1e-30)
    step = jnp.floor(8.0 * jnp.log2(top)) + 2.0
    scale = jnp.exp2(step * -0.125) * 32767.0
    first = place * PACKED
    for m, pair in enumerate(sides):
        low, high = (jnp.round(side * scale).astype(jnp.int32) for side in pair)
        out[first + 8 * m : first + 8 * m + 8, :] = (low & 0xFFFF) | (high << 16)
    out[first + 32 : first + 36, :] = jnp.broadcast_to(step.astype(jnp.int32), (4, LANES))


def sum_products(arrived):
    total = [[0.0, 0.0] for _ in range(4)]
    for place in range(arrived.shape[0] // PACKED):
        first = place * PACKED
        step = arrived[first + 32 : first + 33, :].astype(jnp.float32)
        scale = jnp.exp2(step * 0.125) * (1.0 / 32767.0)
        for m in range(4):
            word = arrived[first + 8 * m : first + 8 * m + 8, :]
            total[m][0] = total[m][0] + ((word << 16) >> 16).astype(jnp.float32) * scale
            total[m][1] = total[m][1] + (word >> 16).astype(jnp.float32) * scale
    return jnp.concatenate([jnp.concatenate(pair, 1) for pair in total], 0)


def add_products(arrived, out):
    total = sum_products(arrived)
    put_products(out, 0, total)
    for place in range(1, out.shape[0] // PACKED):
        out[place * PACKED : (place + 1) * PACKED, :] = out[0:PACKED, :]


def normalize(live_count, sums, node_total, embedded, out):
    total = node_total[...]
    scaled = jnp.sum(sums[...], 0) / total
    mean, square = scaled[0:4, :], scaled[4:8, :]
    dev = jnp.sqrt(square - mean * mean + 1e-05)
    slot = lax.broadcasted_iota(jnp.int32, (embedded.shape[0], 1), 0)
    live = slot < live_count[0]
    for part in range(4):
        columns = slice(part * LANES, (part + 1) * LANES)
        value = (embedded[:, columns] - mean[part : part + 1, :]) / dev[part : part + 1, :]
        out[:, columns] = jnp.where(live, value, 0.0).astype(jnp.bfloat16)


def correlate(core, own, other, normed, out):
    half = normed.shape[2]
    width = 2 * half
    groups, depth, wide = out.shape[0] // PACKED, 8, 4
    contract = (((0,), (0,)), ((), ()))

    def give(left, right):
        product = lax.dot_general(left, right, contract, preferred_element_type=jnp.float32)
        for group in range(groups):
            rows = []
            for n1 in range(depth):
                first = ((group // wide) * depth * wide + n1 * wide + group % wide) * 4
                rows.append(product[first : first + 4, :])
            put_products(out, group, jnp.concatenate(rows, 0))

    @pl.when(core[0] == 0)
    def _():
        normed[0] = own[:, 0:half]
        normed[1] = other[:, half:width]
        give(own[...], other[:, half:width])

    @pl.when(core[0] == 1)
    def _():
        normed[0] = other[:, half:width]
        normed[1] = own[:, 0:half]
        give(other[...], own[:, 0:half])


def finish(core, node, arrived, node_total, correlation, loss):
    half = correlation.shape[1]
    share, depth, wide = 4, 8, 4
    n0, n1, n2 = node[0] // (depth * wide), (node[0] // wide) % depth, node[0] % wide
    value = sum_products(arrived) / node_total[0:1, 0:1]
    place = lax.broadcasted_iota(jnp.int32, value.shape, 0)
    row = ((n0 * depth + place // share) * wide + n2) * share + place % share
    column = lax.broadcasted_iota(jnp.int32, value.shape, 1) + core[0] * half
    mine = value[0:share, :]
    for other in range(1, depth):
        mine = jnp.where(n1 == other, value[other * share : (other + 1) * share, :], mine)
    correlation[...] = mine
    terms = jnp.where(row == column, jnp.square(1.0 - value), 0.005 * jnp.square(value))
    terms = jnp.sum(jnp.sum(terms, 1, keepdims=True), 0, keepdims=True)
    loss[...] = jnp.broadcast_to(terms[None], loss.shape)


def per_device(
    features, row_counts, send_rows, edge_src, edge_dst, edge_keep, w_first, b_first, w_second
):
    local, f_in = features.shape
    peers, halo = send_rows.shape[1], send_rows.shape[2]
    edges = edge_src.shape[1]
    tiles = local // TILE
    half = w_first.shape[1]
    width = 2 * half
    f32, bf16, i32 = jnp.float32, jnp.bfloat16, jnp.int32
    shape = jax.ShapeDtypeStruct
    core_index = lax.axis_index("feat")
    node_index = lax.axis_index(NODES)
    core = core_index.reshape(1).astype(i32)
    node = node_index.reshape(1).astype(i32)
    swap = [(0, 1), (1, 0)]
    planes, depth = lax.axis_size(PLANE), lax.axis_size("nodes_1")

    def partner(value):
        return lax.ppermute(value, "feat", swap)

    first_cores = [2 * peer for peer in range(peers)]
    second_cores = [2 * peer + 1 for peer in reversed(range(peers))]

    def over_nodes(blocks):
        return lax.all_to_all(
            blocks,
            NODES_FEAT,
            split_axis=0,
            concat_axis=0,
            axis_index_groups=[first_cores, second_cores],
            tiled=True,
        )

    def sum_over_nodes(blocks):
        blocks = lax.all_to_all(blocks, PLANE, split_axis=0, concat_axis=0, tiled=True)
        copies = call(
            add_and_copy, shape((depth, *blocks.shape[1:]), f32), [], blocks, name="add_sums"
        )
        return lax.all_to_all(copies, "nodes_1", split_axis=0, concat_axis=0, tiled=True)

    w1_other, w2_other = partner(w_first), partner(w_second)
    bias = b_first.reshape(1, half)
    bias_other = partner(bias)
    outbound = send_rows.reshape(peers * halo)
    sources = lax.dynamic_index_in_dim(edge_src, core_index, 0, False)
    targets = lax.dynamic_index_in_dim(edge_dst, core_index, 0, False)
    kept = lax.dynamic_index_in_dim(edge_keep, core_index, 0, False)
    targets = jnp.where(kept == 1, targets, -1).reshape(tiles, edges // tiles)

    rows_half = peers * halo // 2
    sent, wide = call(
        send_features,
        (shape((rows_half, f_in), bf16), shape((local, f_in), f32)),
        [pltpu.VMEM((rows_half, f_in), f32)],
        features,
        scalars=(core, outbound),
        name="send_features",
    )
    sent, w1_other, w2_other, bias_other = lax.optimization_barrier(
        (sent, w1_other, w2_other, bias_other)
    )
    got = over_nodes(sent.reshape(peers, halo // 2, f_in))
    got_other = partner(got)
    remote = sources - local
    slot_half = (remote % halo) // (halo // 2)
    from_other = (slot_half != core_index).astype(i32)
    sender = jnp.where(slot_half == 1, peers - 1 - remote // halo, remote // halo)
    remote = sender * (halo // 2) + remote % (halo // 2) + from_other * rows_half
    first_sources = jnp.where(sources < local, sources, remote + local)
    mixed, words = call(
        first_mix,
        (shape((local, f_in), f32), shape((peers * PACKED, f_in), i32)),
        [
            pltpu.VMEM((local + 2 * rows_half, f_in), f32),
            pltpu.VMEM((edges // tiles, f_in), f32),
            pltpu.VMEM((edges // tiles, f_in), f32),
            pltpu.VMEM((local, f_in), i32),
            pltpu.VMEM((2 * halo, f_in), i32),
            pltpu.VMEM((2 * halo, f_in), i32),
        ],
        wide,
        got.reshape(rows_half, f_in),
        got_other.reshape(rows_half, f_in),
        targets,
        scalars=(core, row_counts, first_sources, outbound),
        name="first_mix",
    )
    arrived = over_nodes(words.reshape(peers * PACKED // 4, 4, f_in))
    embedded, sums, node_total = call(
        second_mix,
        (
            shape((local, width), f32),
            shape((planes, 8, LANES), f32),
            shape((8, LANES), f32),
        ),
        [
            pltpu.VMEM((local + peers * halo, f_in), f32),
            pltpu.VMEM((TILE + edges // tiles, f_in), f32),
            pltpu.VMEM((TILE + edges // tiles, f_in), f32),
            pltpu.VMEM((3 * f_in, width), bf16),
            pltpu.VMEM((width, width), bf16),
        ],
        arrived.reshape(peers * PACKED, f_in),
        mixed,
        targets,
        w_first,
        w1_other,
        bias,
        bias_other,
        w_second,
        w2_other,
        scalars=(core, row_counts, sources),
        name="second_mix",
    )
    sums = sum_over_nodes(sums)
    own = call(
        normalize,
        shape((local, width), bf16),
        [],
        sums,
        node_total,
        embedded,
        scalars=(row_counts,),
        name="normalize",
    )
    normed, partial = call(
        correlate,
        (shape((2, local, half), bf16), shape((planes * PACKED, LANES), i32)),
        [],
        own,
        partner(own),
        scalars=(core,),
        name="correlate",
    )
    partial = lax.all_to_all(
        partial.reshape(planes * PACKED // 4, 4, LANES), PLANE, split_axis=0, concat_axis=0, tiled=True
    )
    partial = call(
        add_products,
        shape((depth * PACKED, LANES), i32),
        [],
        partial.reshape(planes * PACKED, LANES),
        name="add_products",
    )
    partial = lax.all_to_all(
        partial.reshape(depth * PACKED // 4, 4, LANES), "nodes_1", split_axis=0, concat_axis=0, tiled=True
    )
    partial = partial.reshape(depth * PACKED, LANES)
    devices = lax.axis_size(PLANE_FEAT)
    correlation, loss = call(
        finish,
        (shape((width // peers, half), f32), shape((devices, 1, LANES), f32)),
        [],
        partial,
        node_total,
        scalars=(core, node),
        name="finish",
    )
    losses = lax.all_to_all(loss, PLANE_FEAT, 0, 0, tiled=True)
    return (normed, correlation, jnp.sum(losses[:, 0, 0]))


def solution(mesh):
    torus = Mesh(
        mesh.devices.reshape(4, 8, 4, mesh.shape["feat"]), ("nodes_0", "nodes_1", "nodes_2", "feat")
    )
    placed = (
        P(NODES, None),
        P(NODES),
        P(NODES, None, None),
        P(None, NODES),
        P(None, NODES),
        P(None, NODES),
        P(None, "feat"),
        P("feat"),
        P(None, "feat"),
    )
    return jax.shard_map(
        per_device,
        mesh=torus,
        in_specs=placed,
        out_specs=(P(None, NODES, "feat"), P(NODES, "feat"), P()),
        check_vma=False,
    )
```

```python
import functools

import jax
import jax.numpy as jnp
from jax import lax
from jax.experimental import pallas as pl
from jax.experimental.pallas import tpu as pltpu
from jax.sharding import Mesh
from jax.sharding import PartitionSpec as P

NODES = ("nodes_0", "nodes_1", "nodes_2")
PLANE = ("nodes_0", "nodes_2")
PLANE_FEAT = ("nodes_0", "nodes_2", "feat")
NODES_FEAT = ("nodes_0", "nodes_1", "nodes_2", "feat")

LANES = 128
TILE = 128
CODE_BITS = 17
CODE_TOP = 2 ** (CODE_BITS - 1)
SCALE_BIAS = 224.0
COARSE = 9
PACKED = 34
PRODUCTS = 36

VMEM = pl.BlockSpec(memory_space=pltpu.VMEM)
SMEM = pl.BlockSpec(memory_space=pltpu.SMEM)


def call(body, outs, scratch, *operands, scalars=(), name):
    return pl.pallas_call(
        body,
        out_shape=outs,
        in_specs=[SMEM] * len(scalars) + [VMEM] * len(operands),
        out_specs=jax.tree.map(lambda _: VMEM, outs),
        scratch_shapes=scratch,
        compiler_params=pltpu.CompilerParams(vmem_limit_bytes=26 * 2**20),
        name=name,
    )(*scalars, *operands)


def in_chunks(total, size, body):
    def step(block, _):
        body(pl.multiple_of(block * size, size))
        return 0

    lax.fori_loop(0, total // size, step, 0)


def edge_table(targets, tile):
    inside = targets[tile : tile + 1, :] - tile * TILE
    row = lax.broadcasted_iota(jnp.int32, (TILE, targets.shape[1]), 0)
    table = jnp.where(inside == row, 1.0, 0.0)
    return table.astype(jnp.bfloat16), jnp.sum(table, 1, keepdims=True)


def place_of(core, peer, peers):
    return jnp.where(core[0] == 0, peer, peers - 1 - peer)


def send_features(core, outbound, features, out, table, rows):
    table[...] = features[...].astype(jnp.float32)
    half = out.shape[0] // LANES
    first = core[0] * half

    def step(block, _):
        place = place_of(core, block, out.shape[0] // (4 * half))
        base = pl.multiple_of(place * 4 * half, 4 * half)
        for peer in range(4):
            to = base + jnp.where(core[0] == 0, peer, 3 - peer) * half
            for slot in range(half):
                near = outbound.at[pl.ds(peer * 2 * half + slot, outbound.shape[0] - 8 * half)]
                source = near[block * (8 * half) + first]
                rows[pl.ds(to + slot, 1), :] = table[pl.ds(source, 1), :]
        return 0

    lax.fori_loop(0, out.shape[0] // (4 * half), step, 0)

    def narrow(base):
        out[pl.ds(base, 256), :] = rows[pl.ds(base, 256), :].astype(jnp.bfloat16)

    in_chunks(out.shape[0], 256, narrow)


def first_mix(
    core,
    live_count,
    sources,
    outbound,
    features,
    own,
    other,
    targets,
    mixed,
    words,
    table,
    picked,
    codes,
    coded_even,
    coded_odd,
):
    local = features.shape[0]
    halo = own.shape[0]
    table[0:local, :] = features[...]

    def widen(base):
        table[pl.ds(local + base, 256), :] = own[pl.ds(base, 256), :].astype(jnp.float32)
        table[pl.ds(local + halo + base, 256), :] = other[pl.ds(base, 256), :].astype(jnp.float32)

    in_chunks(halo, 256, widen)
    edges = targets.shape[1]

    def pick(block, _):
        base = pl.multiple_of(block * 128, 128)
        for edge in range(128):
            near = sources.at[pl.ds(edge, sources.shape[0] - 128)]
            picked[pl.ds(base + edge, 1), :] = table[pl.ds(near[base], 1), :]
        return 0

    lax.fori_loop(0, sources.shape[0] // 128, pick, 0)
    for tile in range(local // TILE):
        onehot, degree = edge_table(targets, tile)
        summed = jnp.dot(
            onehot,
            picked[tile * edges : (tile + 1) * edges, :].astype(jnp.bfloat16),
            preferred_element_type=jnp.float32,
        )
        rows = slice(tile * TILE, (tile + 1) * TILE)
        mix = (table[rows, :] + summed) / (1.0 + degree)
        mixed[rows, :] = mix
        top = jnp.maximum(jnp.max(jnp.abs(mix), 1, keepdims=True), 1e-30)
        step = jnp.clip(jnp.floor(8.0 * jnp.log2(top)) + (2.0 + SCALE_BIAS), 0.0, 255.0)
        code = jnp.round(mix * (jnp.exp2((SCALE_BIAS - step) * 0.125) * CODE_TOP))
        code = jnp.clip(code, -CODE_TOP, CODE_TOP - 1).astype(jnp.int32)
        codes[rows, :] = (code & (2**CODE_BITS - 1)) | (step.astype(jnp.int32) << CODE_BITS)

    lane = lax.broadcasted_iota(jnp.int32, (8, LANES), 1)
    row = lax.broadcasted_iota(jnp.int32, (8, LANES), 0)
    counted = jnp.where((lane == COARSE - 1) & (row == 0), live_count[0], 0)

    def pick_slots(block, side, coded):
        for slot in range(128):
            near = outbound.at[pl.ds(side * 128 + slot, outbound.shape[0] - 255)]
            coded[slot : slot + 1, :] = codes[pl.ds(near[block * 256], 1), :]

    def pack(peer, first, coded):
        to = place_of(core, peer, words.shape[0] // PACKED) * PACKED
        octet = [coded[first + 8 * k : first + 8 * k + 8, :] for k in range(8)]
        for k in range(4):
            low = (octet[k] >> 1) & 0xFFFF
            words[pl.ds(to + 8 * k, 8), :] = low | ((octet[k + 4] >> 1) << 16)
        fine = jnp.zeros((8, LANES), jnp.int32)
        coarse = counted
        for k in range(8):
            fine = fine | ((octet[k] & 1) << (4 * k + row // 2))
            scale = (octet[k] >> CODE_BITS) << (8 * (row // 2))
            coarse = coarse | jnp.where(lane == k, scale, 0)
        fine = jnp.where(lane < COARSE, coarse, fine)
        fine = fine | pltpu.roll(fine, 4, 0)
        fine = fine | pltpu.roll(fine, 2, 0)
        words[pl.ds(to + 32, 2), :] = fine[0:2, :]

    blocks = words.shape[0] // (4 * PACKED)
    pick_slots(0, 0, coded_even)

    def both(block, _):
        pick_slots(block, 1, coded_odd)
        pack(block * 4, 0, coded_even)
        pack(block * 4 + 1, 64, coded_even)
        pick_slots(jnp.minimum(block + 1, blocks - 1), 0, coded_even)
        pack(block * 4 + 2, 0, coded_odd)
        pack(block * 4 + 3, 64, coded_odd)
        return 0

    lax.fori_loop(0, blocks, both, 0)


def split_three(value):
    first = value.astype(jnp.bfloat16)
    rest = value - first.astype(jnp.float32)
    second = rest.astype(jnp.bfloat16)
    third = (rest - second.astype(jnp.float32)).astype(jnp.bfloat16)
    return first, second, third


def second_mix(
    core,
    live_count,
    sources,
    words,
    mixed,
    targets,
    w1_own,
    w1_other,
    b_own,
    b_other,
    w2_own,
    w2_other,
    embedded,
    sums,
    node_total,
    table,
    picked_even,
    picked_odd,
    w1,
    w2,
):
    local = mixed.shape[0]
    half = w1_own.shape[1]
    me = core[0]
    mine = pl.multiple_of(me * half, half)
    theirs = pl.multiple_of((1 - me) * half, half)
    for piece in range(3):
        w1[piece * LANES : (piece + 1) * LANES, 0:half] = w1_own[...]
        w1[piece * LANES : (piece + 1) * LANES, half : 2 * half] = w1_other[...]
    w2[0:half, 0:half] = w2_own[pl.ds(mine, half), :]
    w2[half : 2 * half, 0:half] = w2_own[pl.ds(theirs, half), :]
    w2[0:half, half : 2 * half] = w2_other[pl.ds(mine, half), :]
    w2[half : 2 * half, half : 2 * half] = w2_other[pl.ds(theirs, half), :]
    bias = jnp.concatenate([b_own[...], b_other[...]], 1)

    table[0:local, :] = mixed[...]

    lane = lax.broadcasted_iota(jnp.int32, (8, LANES), 1)
    row = lax.broadcasted_iota(jnp.int32, (8, LANES), 0)

    def unpack(peer):
        base = peer * PACKED
        to = place_of(core, peer, words.shape[0] // PACKED) * 64
        to = pl.multiple_of(local + to, 64)
        pairs = [words[pl.ds(base + 8 * k, 8), :] for k in range(4)]
        rest = words[pl.ds(base + 26, 8), :]
        rest = jnp.where(row < 6, pltpu.roll(rest, 6, 0), rest)
        rest = jnp.where(row < 4, pltpu.roll(rest, 4, 0), rest)
        step = (rest >> (8 * (row // 2))) & 255
        scale = jnp.exp2((step.astype(jnp.float32) - SCALE_BIAS) * 0.125) * (1.0 / CODE_TOP)
        fine = jnp.where(lane < COARSE, 0, rest)
        for k in range(8):
            high = (pairs[k] << 16) >> 16 if k < 4 else pairs[k - 4] >> 16
            code = (high << 1) | ((fine >> (4 * k + row // 2)) & 1)
            table[pl.ds(to + 8 * k, 8), :] = code.astype(jnp.float32) * scale[:, k : k + 1]
        return rest

    def unpack_several(block, counts):
        for one in range(8):
            counts = counts + unpack(block * 8 + one)
        return counts

    counts = lax.fori_loop(
        0, words.shape[0] // (8 * PACKED), unpack_several, jnp.zeros((8, LANES), jnp.int32)
    )
    counts = jnp.where((lane == COARSE - 1) & (row == 0), counts, 0).astype(jnp.float32)
    counts = jnp.sum(jnp.sum(counts, 1, keepdims=True), 0, keepdims=True)
    node_total[...] = jnp.broadcast_to(counts, node_total.shape)
    edges = targets.shape[1]
    total = jnp.zeros((1, 2 * half), jnp.float32)
    squares = jnp.zeros((1, 2 * half), jnp.float32)

    def pick(tile, picked):
        picked[0:TILE, :] = mixed[tile * TILE : (tile + 1) * TILE, :]
        for edge in range(edges):
            source = sources[tile * edges + edge]
            picked[TILE + edge : TILE + edge + 1, :] = table[pl.ds(source, 1), :]

    pick(0, picked_even)
    for tile in range(local // TILE):
        rows = slice(tile * TILE, (tile + 1) * TILE)
        picked, later = (picked_even, picked_odd) if tile % 2 == 0 else (picked_odd, picked_even)
        if tile + 1 < local // TILE:
            pick(tile + 1, later)
        value = jnp.concatenate(split_three(picked[...]), 1)
        hidden = jnp.dot(value, w1[...], preferred_element_type=jnp.float32) + bias
        hidden = jnp.maximum(hidden, 0.0).astype(jnp.bfloat16)
        projected = jnp.dot(hidden, w2[...], preferred_element_type=jnp.float32)
        projected = projected.astype(jnp.bfloat16)
        onehot, degree = edge_table(targets, tile)
        summed = jnp.dot(onehot, projected[TILE:, :], preferred_element_type=jnp.float32)
        value = (projected[0:TILE, :].astype(jnp.float32) + summed) / (1.0 + degree)
        embedded[rows, :] = value
        slot = tile * TILE + lax.broadcasted_iota(jnp.int32, (TILE, 1), 0)
        value = jnp.where(slot < live_count[0], value, 0.0)
        total = total + jnp.sum(value, 0, keepdims=True)
        squares = squares + jnp.sum(value * value, 0, keepdims=True)
    for part in range(4):
        columns = slice(part * LANES, (part + 1) * LANES)
        for peer in range(sums.shape[0]):
            sums[peer, part : part + 1, :] = total[:, columns]
            sums[peer, part + 4 : part + 5, :] = squares[:, columns]


def add_and_copy(arrived, out):
    total = arrived[0]
    for peer in range(1, arrived.shape[0]):
        total = total + arrived[peer]
    for peer in range(out.shape[0]):
        out[peer] = total


def put_products(out, place, values):
    sides = [[values[8 * m : 8 * m + 8, side : side + LANES] for side in (0, LANES)] for m in range(4)]
    top = jnp.zeros((8, LANES), jnp.float32)
    for pair in sides:
        for side in pair:
            top = jnp.maximum(top, jnp.abs(side))
    top = jnp.maximum(jnp.max(top, 0, keepdims=True), 1e-30)
    step = jnp.floor(8.0 * jnp.log2(top)) + 2.0
    scale = jnp.exp2(step * -0.125) * 32767.0
    first = place * PRODUCTS
    for m, pair in enumerate(sides):
        low, high = (jnp.round(side * scale).astype(jnp.int32) for side in pair)
        out[first + 8 * m : first + 8 * m + 8, :] = (low & 0xFFFF) | (high << 16)
    out[first + 32 : first + 36, :] = jnp.broadcast_to(step.astype(jnp.int32), (4, LANES))


def sum_products(arrived):
    total = [[0.0, 0.0] for _ in range(4)]
    for place in range(arrived.shape[0] // PRODUCTS):
        first = place * PRODUCTS
        step = arrived[first + 32 : first + 33, :].astype(jnp.float32)
        scale = jnp.exp2(step * 0.125) * (1.0 / 32767.0)
        for m in range(4):
            word = arrived[first + 8 * m : first + 8 * m + 8, :]
            total[m][0] = total[m][0] + ((word << 16) >> 16).astype(jnp.float32) * scale
            total[m][1] = total[m][1] + (word >> 16).astype(jnp.float32) * scale
    return jnp.concatenate([jnp.concatenate(pair, 1) for pair in total], 0)


def add_products(arrived, out):
    total = sum_products(arrived)
    put_products(out, 0, total)
    for place in range(1, out.shape[0] // PRODUCTS):
        out[place * PRODUCTS : (place + 1) * PRODUCTS, :] = out[0:PRODUCTS, :]


def normalize(live_count, sums, node_total, embedded, out):
    total = node_total[...]
    scaled = jnp.sum(sums[...], 0) / total
    mean, square = scaled[0:4, :], scaled[4:8, :]
    dev = jnp.sqrt(square - mean * mean + 1e-05)
    slot = lax.broadcasted_iota(jnp.int32, (embedded.shape[0], 1), 0)
    live = slot < live_count[0]
    for part in range(4):
        columns = slice(part * LANES, (part + 1) * LANES)
        value = (embedded[:, columns] - mean[part : part + 1, :]) / dev[part : part + 1, :]
        out[:, columns] = jnp.where(live, value, 0.0).astype(jnp.bfloat16)


def correlate(core, own, other, normed, out):
    half = normed.shape[2]
    width = 2 * half
    groups, depth, wide = out.shape[0] // PRODUCTS, 8, 4
    contract = (((0,), (0,)), ((), ()))

    def give(left, right):
        product = lax.dot_general(left, right, contract, preferred_element_type=jnp.float32)
        for group in range(groups):
            rows = []
            for n1 in range(depth):
                first = ((group // wide) * depth * wide + n1 * wide + group % wide) * 4
                rows.append(product[first : first + 4, :])
            put_products(out, group, jnp.concatenate(rows, 0))

    @pl.when(core[0] == 0)
    def _():
        normed[0] = own[:, 0:half]
        normed[1] = other[:, half:width]
        give(own[...], other[:, half:width])

    @pl.when(core[0] == 1)
    def _():
        normed[0] = other[:, half:width]
        normed[1] = own[:, 0:half]
        give(other[...], own[:, 0:half])


def finish(core, node, arrived, node_total, correlation, loss):
    half = correlation.shape[1]
    share, depth, wide = 4, 8, 4
    n0, n1, n2 = node[0] // (depth * wide), (node[0] // wide) % depth, node[0] % wide
    value = sum_products(arrived) / node_total[0:1, 0:1]
    place = lax.broadcasted_iota(jnp.int32, value.shape, 0)
    row = ((n0 * depth + place // share) * wide + n2) * share + place % share
    column = lax.broadcasted_iota(jnp.int32, value.shape, 1) + core[0] * half
    mine = value[0:share, :]
    for other in range(1, depth):
        mine = jnp.where(n1 == other, value[other * share : (other + 1) * share, :], mine)
    correlation[...] = mine
    terms = jnp.where(row == column, jnp.square(1.0 - value), 0.005 * jnp.square(value))
    terms = jnp.sum(jnp.sum(terms, 1, keepdims=True), 0, keepdims=True)
    loss[...] = jnp.broadcast_to(terms[None], loss.shape)


def per_device(
    features, row_counts, send_rows, edge_src, edge_dst, edge_keep, w_first, b_first, w_second
):
    local, f_in = features.shape
    peers, halo = send_rows.shape[1], send_rows.shape[2]
    edges = edge_src.shape[1]
    tiles = local // TILE
    half = w_first.shape[1]
    width = 2 * half
    f32, bf16, i32 = jnp.float32, jnp.bfloat16, jnp.int32
    shape = jax.ShapeDtypeStruct
    core_index = lax.axis_index("feat")
    node_index = lax.axis_index(NODES)
    core = core_index.reshape(1).astype(i32)
    node = node_index.reshape(1).astype(i32)
    swap = [(0, 1), (1, 0)]
    planes, depth = lax.axis_size(PLANE), lax.axis_size("nodes_1")

    def partner(value):
        return lax.ppermute(value, "feat", swap)

    first_cores = [2 * peer for peer in range(peers)]
    second_cores = [2 * peer + 1 for peer in reversed(range(peers))]

    def over_nodes(blocks):
        return lax.all_to_all(
            blocks,
            NODES_FEAT,
            split_axis=0,
            concat_axis=0,
            axis_index_groups=[first_cores, second_cores],
            tiled=True,
        )

    def sum_over_nodes(blocks):
        blocks = lax.all_to_all(blocks, PLANE, split_axis=0, concat_axis=0, tiled=True)
        copies = call(
            add_and_copy, shape((depth, *blocks.shape[1:]), f32), [], blocks, name="add_sums"
        )
        return lax.all_to_all(copies, "nodes_1", split_axis=0, concat_axis=0, tiled=True)

    w1_other, w2_other = partner(w_first), partner(w_second)
    bias = b_first.reshape(1, half)
    bias_other = partner(bias)
    outbound = send_rows.reshape(peers * halo)
    sources = lax.dynamic_index_in_dim(edge_src, core_index, 0, False)
    targets = lax.dynamic_index_in_dim(edge_dst, core_index, 0, False)
    kept = lax.dynamic_index_in_dim(edge_keep, core_index, 0, False)
    targets = jnp.where(kept == 1, targets, -1).reshape(tiles, edges // tiles)

    rows_half = peers * halo // 2
    sent, wide = call(
        send_features,
        (shape((rows_half, f_in), bf16), shape((local, f_in), f32)),
        [pltpu.VMEM((rows_half, f_in), f32)],
        features,
        scalars=(core, outbound),
        name="send_features",
    )
    sent, w1_other, w2_other, bias_other = lax.optimization_barrier(
        (sent, w1_other, w2_other, bias_other)
    )
    got = over_nodes(sent.reshape(peers, halo // 2, f_in))
    got_other = partner(got)
    remote = sources - local
    slot_half = (remote % halo) // (halo // 2)
    from_other = (slot_half != core_index).astype(i32)
    sender = jnp.where(slot_half == 1, peers - 1 - remote // halo, remote // halo)
    remote = sender * (halo // 2) + remote % (halo // 2) + from_other * rows_half
    first_sources = jnp.where(sources < local, sources, remote + local)
    mixed, words = call(
        first_mix,
        (shape((local, f_in), f32), shape((peers * PACKED, f_in), i32)),
        [
            pltpu.VMEM((local + 2 * rows_half, f_in), f32),
            pltpu.VMEM((edges, f_in), f32),
            pltpu.VMEM((local, f_in), i32),
            pltpu.VMEM((2 * halo, f_in), i32),
            pltpu.VMEM((2 * halo, f_in), i32),
        ],
        wide,
        got.reshape(rows_half, f_in),
        got_other.reshape(rows_half, f_in),
        targets,
        scalars=(core, row_counts, first_sources, outbound),
        name="first_mix",
    )
    arrived = over_nodes(words.reshape(peers * PACKED // 2, 2, f_in))
    embedded, sums, node_total = call(
        second_mix,
        (
            shape((local, width), f32),
            shape((planes, 8, LANES), f32),
            shape((8, LANES), f32),
        ),
        [
            pltpu.VMEM((local + peers * halo, f_in), f32),
            pltpu.VMEM((TILE + edges // tiles, f_in), f32),
            pltpu.VMEM((TILE + edges // tiles, f_in), f32),
            pltpu.VMEM((3 * f_in, width), bf16),
            pltpu.VMEM((width, width), bf16),
        ],
        arrived.reshape(peers * PACKED, f_in),
        mixed,
        targets,
        w_first,
        w1_other,
        bias,
        bias_other,
        w_second,
        w2_other,
        scalars=(core, row_counts, sources),
        name="second_mix",
    )
    sums = sum_over_nodes(sums)
    own = call(
        normalize,
        shape((local, width), bf16),
        [],
        sums,
        node_total,
        embedded,
        scalars=(row_counts,),
        name="normalize",
    )
    normed, partial = call(
        correlate,
        (shape((2, local, half), bf16), shape((planes * PRODUCTS, LANES), i32)),
        [],
        own,
        partner(own),
        scalars=(core,),
        name="correlate",
    )
    partial = lax.all_to_all(
        partial.reshape(planes * PRODUCTS // 4, 4, LANES), PLANE, split_axis=0, concat_axis=0, tiled=True
    )
    partial = call(
        add_products,
        shape((depth * PRODUCTS, LANES), i32),
        [],
        partial.reshape(planes * PRODUCTS, LANES),
        name="add_products",
    )
    partial = lax.all_to_all(
        partial.reshape(depth * PRODUCTS // 4, 4, LANES), "nodes_1", split_axis=0, concat_axis=0, tiled=True
    )
    partial = partial.reshape(depth * PRODUCTS, LANES)
    devices = lax.axis_size(PLANE_FEAT)
    correlation, loss = call(
        finish,
        (shape((width // peers, half), f32), shape((devices, 1, LANES), f32)),
        [],
        partial,
        node_total,
        scalars=(core, node),
        name="finish",
    )
    losses = lax.all_to_all(loss, PLANE_FEAT, 0, 0, tiled=True)
    return (normed, correlation, jnp.sum(losses[:, 0, 0]))


def solution(mesh):
    torus = Mesh(
        mesh.devices.reshape(4, 8, 4, mesh.shape["feat"]), ("nodes_0", "nodes_1", "nodes_2", "feat")
    )
    placed = (
        P(NODES, None),
        P(NODES),
        P(NODES, None, None),
        P(None, NODES),
        P(None, NODES),
        P(None, NODES),
        P(None, "feat"),
        P("feat"),
        P(None, "feat"),
    )
    return jax.shard_map(
        per_device,
        mesh=torus,
        in_specs=placed,
        out_specs=(P(None, NODES, "feat"), P(NODES, "feat"), P()),
        check_vma=False,
    )
```

```python
import functools

import jax
import jax.numpy as jnp
from jax import lax
from jax.experimental import pallas as pl
from jax.experimental.pallas import tpu as pltpu
from jax.sharding import Mesh
from jax.sharding import PartitionSpec as P

NODES = ("nodes_0", "nodes_1", "nodes_2")
PLANE = ("nodes_0", "nodes_2")
PLANE_FEAT = ("nodes_0", "nodes_2", "feat")
NODES_FEAT = ("nodes_0", "nodes_1", "nodes_2", "feat")

LANES = 128
TILE = 128
CODE_BITS = 17
CODE_TOP = 2 ** (CODE_BITS - 1)
SCALE_BIAS = 224.0
COARSE = 9
PACKED = 34
PRODUCTS = 36

VMEM = pl.BlockSpec(memory_space=pltpu.VMEM)
SMEM = pl.BlockSpec(memory_space=pltpu.SMEM)


def call(body, outs, scratch, *operands, scalars=(), name):
    return pl.pallas_call(
        body,
        out_shape=outs,
        in_specs=[SMEM] * len(scalars) + [VMEM] * len(operands),
        out_specs=jax.tree.map(lambda _: VMEM, outs),
        scratch_shapes=scratch,
        compiler_params=pltpu.CompilerParams(vmem_limit_bytes=26 * 2**20),
        name=name,
    )(*scalars, *operands)


def in_chunks(total, size, body):
    def step(block, _):
        body(pl.multiple_of(block * size, size))
        return 0

    lax.fori_loop(0, total // size, step, 0)


def edge_table(targets, tile):
    inside = targets[tile : tile + 1, :] - tile * TILE
    row = lax.broadcasted_iota(jnp.int32, (TILE, targets.shape[1]), 0)
    table = jnp.where(inside == row, 1.0, 0.0)
    return table.astype(jnp.bfloat16), jnp.sum(table, 1, keepdims=True)


FOUR = 4


def send_features(core, outbound, table, out, rows):
    half = out.shape[0] // LANES
    first = core[0] * half

    def step(block, _):
        place = jnp.where(core[0] == 0, block, out.shape[0] // (FOUR * half) - 1 - block)
        base = pl.multiple_of(place * FOUR * half, FOUR * half)
        for peer in range(FOUR):
            for slot in range(half):
                near = outbound.at[pl.ds(peer * 2 * half + slot, outbound.shape[0] - 8 * half)]
                source = near[block * (8 * half) + first]
                rows[pl.ds(base + peer * half + slot, 1), :] = table[pl.ds(source, 1), :]
        return 0

    lax.fori_loop(0, out.shape[0] // (4 * half), step, 0)

    def narrow(base):
        out[pl.ds(base, 256), :] = rows[pl.ds(base, 256), :].astype(jnp.bfloat16)

    in_chunks(out.shape[0], 256, narrow)


def first_mix(
    live_count,
    sources,
    outbound,
    features,
    own,
    other,
    targets,
    mixed,
    words,
    table,
    picked,
    codes,
    coded_even,
    coded_odd,
):
    local = features.shape[0]
    halo = own.shape[0]
    table[0:local, :] = features[...]

    def widen(base):
        table[pl.ds(local + base, 256), :] = own[pl.ds(base, 256), :].astype(jnp.float32)
        table[pl.ds(local + halo + base, 256), :] = other[pl.ds(base, 256), :].astype(jnp.float32)

    in_chunks(halo, 256, widen)
    edges = targets.shape[1]

    def pick(block, _):
        base = pl.multiple_of(block * 128, 128)
        for edge in range(128):
            near = sources.at[pl.ds(edge, sources.shape[0] - 128)]
            picked[pl.ds(base + edge, 1), :] = table[pl.ds(near[base], 1), :]
        return 0

    lax.fori_loop(0, sources.shape[0] // 128, pick, 0)
    for tile in range(local // TILE):
        onehot, degree = edge_table(targets, tile)
        summed = jnp.dot(
            onehot,
            picked[tile * edges : (tile + 1) * edges, :].astype(jnp.bfloat16),
            preferred_element_type=jnp.float32,
        )
        rows = slice(tile * TILE, (tile + 1) * TILE)
        mix = (table[rows, :] + summed) / (1.0 + degree)
        mixed[rows, :] = mix
        top = jnp.maximum(jnp.max(jnp.abs(mix), 1, keepdims=True), 1e-30)
        step = jnp.clip(jnp.floor(8.0 * jnp.log2(top)) + (2.0 + SCALE_BIAS), 0.0, 255.0)
        code = jnp.round(mix * (jnp.exp2((SCALE_BIAS - step) * 0.125) * CODE_TOP))
        code = jnp.clip(code, -CODE_TOP, CODE_TOP - 1).astype(jnp.int32)
        codes[rows, :] = (code & (2**CODE_BITS - 1)) | (step.astype(jnp.int32) << CODE_BITS)

    lane = lax.broadcasted_iota(jnp.int32, (8, LANES), 1)
    row = lax.broadcasted_iota(jnp.int32, (8, LANES), 0)
    counted = jnp.where((lane == COARSE - 1) & (row == 0), live_count[0], 0)

    def pick_slots(block, side, coded):
        for slot in range(128):
            near = outbound.at[pl.ds(side * 128 + slot, outbound.shape[0] - 255)]
            coded[slot : slot + 1, :] = codes[pl.ds(near[block * 256], 1), :]

    def pack(peer, first, coded):
        to = peer * PACKED
        octet = [coded[first + 8 * k : first + 8 * k + 8, :] for k in range(8)]
        for k in range(4):
            low = (octet[k] >> 1) & 0xFFFF
            words[pl.ds(to + 8 * k, 8), :] = low | ((octet[k + 4] >> 1) << 16)
        fine = jnp.zeros((8, LANES), jnp.int32)
        coarse = counted
        for k in range(8):
            fine = fine | ((octet[k] & 1) << (4 * k + row // 2))
            scale = (octet[k] >> CODE_BITS) << (8 * (row // 2))
            coarse = coarse | jnp.where(lane == k, scale, 0)
        fine = jnp.where(lane < COARSE, coarse, fine)
        fine = fine | pltpu.roll(fine, 4, 0)
        fine = fine | pltpu.roll(fine, 2, 0)
        words[pl.ds(to + 32, 2), :] = fine[0:2, :]

    blocks = words.shape[0] // (4 * PACKED)
    pick_slots(0, 0, coded_even)

    def both(block, _):
        pick_slots(block, 1, coded_odd)
        pack(block * 4, 0, coded_even)
        pack(block * 4 + 1, 64, coded_even)
        pick_slots(jnp.minimum(block + 1, blocks - 1), 0, coded_even)
        pack(block * 4 + 2, 0, coded_odd)
        pack(block * 4 + 3, 64, coded_odd)
        return 0

    lax.fori_loop(0, blocks, both, 0)


def split_three(value):
    first = value.astype(jnp.bfloat16)
    rest = value - first.astype(jnp.float32)
    second = rest.astype(jnp.bfloat16)
    third = (rest - second.astype(jnp.float32)).astype(jnp.bfloat16)
    return first, second, third


def second_mix(
    core,
    live_count,
    sources,
    words,
    mixed,
    targets,
    w1_own,
    w1_other,
    b_own,
    b_other,
    w2_own,
    w2_other,
    embedded,
    sums,
    node_total,
    table,
    picked_even,
    picked_odd,
    w1,
    w2,
):
    local = mixed.shape[0]
    half = w1_own.shape[1]
    me = core[0]
    mine = pl.multiple_of(me * half, half)
    theirs = pl.multiple_of((1 - me) * half, half)
    for piece in range(3):
        w1[piece * LANES : (piece + 1) * LANES, 0:half] = w1_own[...]
        w1[piece * LANES : (piece + 1) * LANES, half : 2 * half] = w1_other[...]
    w2[0:half, 0:half] = w2_own[pl.ds(mine, half), :]
    w2[half : 2 * half, 0:half] = w2_own[pl.ds(theirs, half), :]
    w2[0:half, half : 2 * half] = w2_other[pl.ds(mine, half), :]
    w2[half : 2 * half, half : 2 * half] = w2_other[pl.ds(theirs, half), :]
    bias = jnp.concatenate([b_own[...], b_other[...]], 1)

    table[0:local, :] = mixed[...]

    lane = lax.broadcasted_iota(jnp.int32, (8, LANES), 1)
    row = lax.broadcasted_iota(jnp.int32, (8, LANES), 0)

    def unpack(peer):
        base = peer * PACKED
        to = pl.multiple_of(local + peer * 64, 64)
        pairs = [words[pl.ds(base + 8 * k, 8), :] for k in range(4)]
        rest = words[pl.ds(base + 26, 8), :]
        rest = jnp.where(row < 6, pltpu.roll(rest, 6, 0), rest)
        rest = jnp.where(row < 4, pltpu.roll(rest, 4, 0), rest)
        step = (rest >> (8 * (row // 2))) & 255
        scale = jnp.exp2((step.astype(jnp.float32) - SCALE_BIAS) * 0.125) * (1.0 / CODE_TOP)
        fine = jnp.where(lane < COARSE, 0, rest)
        for k in range(8):
            high = (pairs[k] << 16) >> 16 if k < 4 else pairs[k - 4] >> 16
            code = (high << 1) | ((fine >> (4 * k + row // 2)) & 1)
            table[pl.ds(to + 8 * k, 8), :] = code.astype(jnp.float32) * scale[:, k : k + 1]
        return rest

    def unpack_several(block, counts):
        for one in range(16):
            counts = counts + unpack(block * 16 + one)
        return counts

    counts = lax.fori_loop(
        0, words.shape[0] // (16 * PACKED), unpack_several, jnp.zeros((8, LANES), jnp.int32)
    )
    counts = jnp.where((lane == COARSE - 1) & (row == 0), counts, 0).astype(jnp.float32)
    counts = jnp.sum(jnp.sum(counts, 1, keepdims=True), 0, keepdims=True)
    node_total[...] = jnp.broadcast_to(counts, node_total.shape)
    edges = targets.shape[1]
    total = jnp.zeros((1, 2 * half), jnp.float32)
    squares = jnp.zeros((1, 2 * half), jnp.float32)

    def pick(tile, picked):
        picked[0:TILE, :] = mixed[tile * TILE : (tile + 1) * TILE, :]
        for edge in range(edges):
            source = sources[tile * edges + edge]
            picked[TILE + edge : TILE + edge + 1, :] = table[pl.ds(source, 1), :]

    pick(0, picked_even)
    for tile in range(local // TILE):
        rows = slice(tile * TILE, (tile + 1) * TILE)
        picked, later = (picked_even, picked_odd) if tile % 2 == 0 else (picked_odd, picked_even)
        if tile + 1 < local // TILE:
            pick(tile + 1, later)
        value = jnp.concatenate(split_three(picked[...]), 1)
        hidden = jnp.dot(value, w1[...], preferred_element_type=jnp.float32) + bias
        hidden = jnp.maximum(hidden, 0.0).astype(jnp.bfloat16)
        projected = jnp.dot(hidden, w2[...], preferred_element_type=jnp.float32)
        projected = projected.astype(jnp.bfloat16)
        onehot, degree = edge_table(targets, tile)
        summed = jnp.dot(onehot, projected[TILE:, :], preferred_element_type=jnp.float32)
        value = (projected[0:TILE, :].astype(jnp.float32) + summed) / (1.0 + degree)
        embedded[rows, :] = value
        slot = tile * TILE + lax.broadcasted_iota(jnp.int32, (TILE, 1), 0)
        value = jnp.where(slot < live_count[0], value, 0.0)
        total = total + jnp.sum(value, 0, keepdims=True)
        squares = squares + jnp.sum(value * value, 0, keepdims=True)
    for part in range(4):
        columns = slice(part * LANES, (part + 1) * LANES)
        for peer in range(sums.shape[0]):
            sums[peer, part : part + 1, :] = total[:, columns]
            sums[peer, part + 4 : part + 5, :] = squares[:, columns]


def add_and_copy(arrived, out):
    total = arrived[0]
    for peer in range(1, arrived.shape[0]):
        total = total + arrived[peer]
    for peer in range(out.shape[0]):
        out[peer] = total


def put_products(out, place, values):
    sides = [[values[8 * m : 8 * m + 8, side : side + LANES] for side in (0, LANES)] for m in range(4)]
    top = jnp.zeros((8, LANES), jnp.float32)
    for pair in sides:
        for side in pair:
            top = jnp.maximum(top, jnp.abs(side))
    top = jnp.maximum(jnp.max(top, 0, keepdims=True), 1e-30)
    step = jnp.floor(8.0 * jnp.log2(top)) + 2.0
    scale = jnp.exp2(step * -0.125) * 32767.0
    first = place * PRODUCTS
    for m, pair in enumerate(sides):
        low, high = (jnp.round(side * scale).astype(jnp.int32) for side in pair)
        out[first + 8 * m : first + 8 * m + 8, :] = (low & 0xFFFF) | (high << 16)
    out[first + 32 : first + 36, :] = jnp.broadcast_to(step.astype(jnp.int32), (4, LANES))


def sum_products(arrived):
    total = [[0.0, 0.0] for _ in range(4)]
    for place in range(arrived.shape[0] // PRODUCTS):
        first = place * PRODUCTS
        step = arrived[first + 32 : first + 33, :].astype(jnp.float32)
        scale = jnp.exp2(step * 0.125) * (1.0 / 32767.0)
        for m in range(4):
            word = arrived[first + 8 * m : first + 8 * m + 8, :]
            total[m][0] = total[m][0] + ((word << 16) >> 16).astype(jnp.float32) * scale
            total[m][1] = total[m][1] + (word >> 16).astype(jnp.float32) * scale
    return jnp.concatenate([jnp.concatenate(pair, 1) for pair in total], 0)


def add_products(arrived, out):
    total = sum_products(arrived)
    put_products(out, 0, total)
    for place in range(1, out.shape[0] // PRODUCTS):
        out[place * PRODUCTS : (place + 1) * PRODUCTS, :] = out[0:PRODUCTS, :]


def normalize(live_count, sums, node_total, embedded, out):
    total = node_total[...]
    scaled = jnp.sum(sums[...], 0) / total
    mean, square = scaled[0:4, :], scaled[4:8, :]
    dev = jnp.sqrt(square - mean * mean + 1e-05)
    slot = lax.broadcasted_iota(jnp.int32, (embedded.shape[0], 1), 0)
    live = slot < live_count[0]
    for part in range(4):
        columns = slice(part * LANES, (part + 1) * LANES)
        value = (embedded[:, columns] - mean[part : part + 1, :]) / dev[part : part + 1, :]
        out[:, columns] = jnp.where(live, value, 0.0).astype(jnp.bfloat16)


def correlate(core, own, other, normed, out):
    half = normed.shape[2]
    width = 2 * half
    groups, depth, wide = out.shape[0] // PRODUCTS, 8, 4
    contract = (((0,), (0,)), ((), ()))

    def give(left, right):
        product = lax.dot_general(left, right, contract, preferred_element_type=jnp.float32)
        for group in range(groups):
            rows = []
            for n1 in range(depth):
                first = ((group // wide) * depth * wide + n1 * wide + group % wide) * 4
                rows.append(product[first : first + 4, :])
            put_products(out, group, jnp.concatenate(rows, 0))

    @pl.when(core[0] == 0)
    def _():
        normed[0] = own[:, 0:half]
        normed[1] = other[:, half:width]
        give(own[...], other[:, half:width])

    @pl.when(core[0] == 1)
    def _():
        normed[0] = other[:, half:width]
        normed[1] = own[:, 0:half]
        give(other[...], own[:, 0:half])


def finish(core, node, arrived, node_total, correlation, loss):
    half = correlation.shape[1]
    share, depth, wide = 4, 8, 4
    n0, n1, n2 = node[0] // (depth * wide), (node[0] // wide) % depth, node[0] % wide
    value = sum_products(arrived) / node_total[0:1, 0:1]
    place = lax.broadcasted_iota(jnp.int32, value.shape, 0)
    row = ((n0 * depth + place // share) * wide + n2) * share + place % share
    column = lax.broadcasted_iota(jnp.int32, value.shape, 1) + core[0] * half
    mine = value[0:share, :]
    for other in range(1, depth):
        mine = jnp.where(n1 == other, value[other * share : (other + 1) * share, :], mine)
    correlation[...] = mine
    terms = jnp.where(row == column, jnp.square(1.0 - value), 0.005 * jnp.square(value))
    terms = jnp.sum(jnp.sum(terms, 1, keepdims=True), 0, keepdims=True)
    loss[...] = jnp.broadcast_to(terms[None], loss.shape)


def per_device(
    features, row_counts, send_rows, edge_src, edge_dst, edge_keep, w_first, b_first, w_second
):
    local, f_in = features.shape
    peers, halo = send_rows.shape[1], send_rows.shape[2]
    edges = edge_src.shape[1]
    tiles = local // TILE
    half = w_first.shape[1]
    width = 2 * half
    f32, bf16, i32 = jnp.float32, jnp.bfloat16, jnp.int32
    shape = jax.ShapeDtypeStruct
    core_index = lax.axis_index("feat")
    node_index = lax.axis_index(NODES)
    core = core_index.reshape(1).astype(i32)
    node = node_index.reshape(1).astype(i32)
    swap = [(0, 1), (1, 0)]
    planes, depth = lax.axis_size(PLANE), lax.axis_size("nodes_1")

    def partner(value):
        return lax.ppermute(value, "feat", swap)

    first_cores = [2 * peer for peer in range(peers)]
    second_cores = [
        2 * (four + peer) + 1 for four in reversed(range(0, peers, FOUR)) for peer in range(FOUR)
    ]

    def sum_over_nodes(blocks):
        blocks = lax.all_to_all(blocks, PLANE, split_axis=0, concat_axis=0, tiled=True)
        copies = call(
            add_and_copy, shape((depth, *blocks.shape[1:]), f32), [], blocks, name="add_sums"
        )
        return lax.all_to_all(copies, "nodes_1", split_axis=0, concat_axis=0, tiled=True)

    w1_other, w2_other = partner(w_first), partner(w_second)
    bias = b_first.reshape(1, half)
    bias_other = partner(bias)
    outbound = send_rows.reshape(peers * halo)
    sources = lax.dynamic_index_in_dim(edge_src, core_index, 0, False)
    targets = lax.dynamic_index_in_dim(edge_dst, core_index, 0, False)
    kept = lax.dynamic_index_in_dim(edge_keep, core_index, 0, False)
    targets = jnp.where(kept == 1, targets, -1).reshape(tiles, edges // tiles)

    rows_half = peers * halo // 2
    wide = features.astype(f32)
    sent = call(
        send_features,
        shape((rows_half, f_in), bf16),
        [pltpu.VMEM((rows_half, f_in), f32)],
        wide,
        scalars=(core, outbound),
        name="send_features",
    )
    sent, w1_other, w2_other, bias_other = lax.optimization_barrier(
        (sent, w1_other, w2_other, bias_other)
    )
    got = lax.all_to_all(
        sent.reshape(peers, halo // 2, f_in),
        NODES_FEAT,
        split_axis=0,
        concat_axis=0,
        axis_index_groups=[first_cores, second_cores],
        tiled=True,
    )
    got_other = partner(got)
    remote = sources - local
    slot_half = (remote % halo) // (halo // 2)
    from_other = (slot_half != core_index).astype(i32)
    sender = remote // halo
    sender = jnp.where(slot_half == 1, peers - FOUR - sender + 2 * (sender % FOUR), sender)
    remote = sender * (halo // 2) + remote % (halo // 2) + from_other * rows_half
    first_sources = jnp.where(sources < local, sources, remote + local)
    mixed, words = call(
        first_mix,
        (shape((local, f_in), f32), shape((peers * PACKED, f_in), i32)),
        [
            pltpu.VMEM((local + 2 * rows_half, f_in), f32),
            pltpu.VMEM((edges, f_in), f32),
            pltpu.VMEM((local, f_in), i32),
            pltpu.VMEM((2 * halo, f_in), i32),
            pltpu.VMEM((2 * halo, f_in), i32),
        ],
        wide,
        got.reshape(rows_half, f_in),
        got_other.reshape(rows_half, f_in),
        targets,
        scalars=(row_counts, first_sources, outbound),
        name="first_mix",
    )
    arrived = lax.all_to_all(
        words.reshape(peers * PACKED // 2, 2, f_in), NODES, split_axis=0, concat_axis=0, tiled=True
    )
    embedded, sums, node_total = call(
        second_mix,
        (
            shape((local, width), f32),
            shape((planes, 8, LANES), f32),
            shape((8, LANES), f32),
        ),
        [
            pltpu.VMEM((local + peers * halo, f_in), f32),
            pltpu.VMEM((TILE + edges // tiles, f_in), f32),
            pltpu.VMEM((TILE + edges // tiles, f_in), f32),
            pltpu.VMEM((3 * f_in, width), bf16),
            pltpu.VMEM((width, width), bf16),
        ],
        arrived.reshape(peers * PACKED, f_in),
        mixed,
        targets,
        w_first,
        w1_other,
        bias,
        bias_other,
        w_second,
        w2_other,
        scalars=(core, row_counts, sources),
        name="second_mix",
    )
    sums = sum_over_nodes(sums)
    own = call(
        normalize,
        shape((local, width), bf16),
        [],
        sums,
        node_total,
        embedded,
        scalars=(row_counts,),
        name="normalize",
    )
    normed, partial = call(
        correlate,
        (shape((2, local, half), bf16), shape((planes * PRODUCTS, LANES), i32)),
        [],
        own,
        partner(own),
        scalars=(core,),
        name="correlate",
    )
    partial = lax.all_to_all(
        partial.reshape(planes * PRODUCTS // 4, 4, LANES), PLANE, split_axis=0, concat_axis=0, tiled=True
    )
    partial = call(
        add_products,
        shape((depth * PRODUCTS, LANES), i32),
        [],
        partial.reshape(planes * PRODUCTS, LANES),
        name="add_products",
    )
    partial = lax.all_to_all(
        partial.reshape(depth * PRODUCTS // 4, 4, LANES), "nodes_1", split_axis=0, concat_axis=0, tiled=True
    )
    partial = partial.reshape(depth * PRODUCTS, LANES)
    devices = lax.axis_size(PLANE_FEAT)
    correlation, loss = call(
        finish,
        (shape((width // peers, half), f32), shape((devices, 1, LANES), f32)),
        [],
        partial,
        node_total,
        scalars=(core, node),
        name="finish",
    )
    losses = lax.all_to_all(loss, PLANE_FEAT, 0, 0, tiled=True)
    return (normed, correlation, jnp.sum(losses[:, 0, 0]))


def solution(mesh):
    torus = Mesh(
        mesh.devices.reshape(4, 8, 4, mesh.shape["feat"]), ("nodes_0", "nodes_1", "nodes_2", "feat")
    )
    placed = (
        P(NODES, None),
        P(NODES),
        P(NODES, None, None),
        P(None, NODES),
        P(None, NODES),
        P(None, NODES),
        P(None, "feat"),
        P("feat"),
        P(None, "feat"),
    )
    return jax.shard_map(
        per_device,
        mesh=torus,
        in_specs=placed,
        out_specs=(P(None, NODES, "feat"), P(NODES, "feat"), P()),
        check_vma=False,
    )
```

```python
import functools

import jax
import jax.numpy as jnp
from jax import lax
from jax.experimental import pallas as pl
from jax.experimental.pallas import tpu as pltpu
from jax.sharding import Mesh
from jax.sharding import PartitionSpec as P

NODES = ("nodes_0", "nodes_1", "nodes_2")
PLANE = ("nodes_0", "nodes_2")
PLANE_FEAT = ("nodes_0", "nodes_2", "feat")
NODES_FEAT = ("nodes_0", "nodes_1", "nodes_2", "feat")

LANES = 128
TILE = 128
CODE_BITS = 17
CODE_TOP = 2 ** (CODE_BITS - 1)
SCALE_BIAS = 224.0
COARSE = 9
PACKED = 34
PRODUCTS = 36

VMEM = pl.BlockSpec(memory_space=pltpu.VMEM)
SMEM = pl.BlockSpec(memory_space=pltpu.SMEM)


def call(body, outs, scratch, *operands, scalars=(), name):
    return pl.pallas_call(
        body,
        out_shape=outs,
        in_specs=[SMEM] * len(scalars) + [VMEM] * len(operands),
        out_specs=jax.tree.map(lambda _: VMEM, outs),
        scratch_shapes=scratch,
        compiler_params=pltpu.CompilerParams(vmem_limit_bytes=26 * 2**20),
        name=name,
    )(*scalars, *operands)


def in_chunks(total, size, body):
    def step(block, _):
        body(pl.multiple_of(block * size, size))
        return 0

    lax.fori_loop(0, total // size, step, 0)


def edge_table(targets, tile):
    inside = targets[tile : tile + 1, :] - tile * TILE
    row = lax.broadcasted_iota(jnp.int32, (TILE, targets.shape[1]), 0)
    table = jnp.where(inside == row, 1.0, 0.0)
    return table.astype(jnp.bfloat16), jnp.sum(table, 1, keepdims=True)


FOUR = 4


def send_features(core, outbound, table, out, rows):
    half = out.shape[0] // LANES
    first = core[0] * half

    def step(block, _):
        place = jnp.where(core[0] == 0, block, out.shape[0] // (FOUR * half) - 1 - block)
        base = pl.multiple_of(place * FOUR * half, FOUR * half)
        for peer in range(FOUR):
            for slot in range(half):
                near = outbound.at[pl.ds(peer * 2 * half + slot, outbound.shape[0] - 8 * half)]
                source = near[block * (8 * half) + first]
                rows[pl.ds(base + peer * half + slot, 1), :] = table[pl.ds(source, 1), :]
        return 0

    lax.fori_loop(0, out.shape[0] // (4 * half), step, 0)

    def narrow(base):
        out[pl.ds(base, 256), :] = rows[pl.ds(base, 256), :].astype(jnp.bfloat16)

    in_chunks(out.shape[0], 256, narrow)


def first_mix(
    live_count,
    sources,
    outbound,
    features,
    own,
    other,
    targets,
    mixed,
    words,
    table,
    picked,
    codes,
    coded_even,
    coded_odd,
):
    local = features.shape[0]
    halo = own.shape[0]
    table[0:local, :] = features[...]

    def widen(base):
        table[pl.ds(local + base, 256), :] = own[pl.ds(base, 256), :].astype(jnp.float32)
        table[pl.ds(local + halo + base, 256), :] = other[pl.ds(base, 256), :].astype(jnp.float32)

    in_chunks(halo, 256, widen)
    edges = targets.shape[1]

    def pick(block, _):
        base = pl.multiple_of(block * 128, 128)
        for edge in range(128):
            near = sources.at[pl.ds(edge, sources.shape[0] - 128)]
            picked[pl.ds(base + edge, 1), :] = table[pl.ds(near[base], 1), :]
        return 0

    lax.fori_loop(0, sources.shape[0] // 128, pick, 0)
    for tile in range(local // TILE):
        onehot, degree = edge_table(targets, tile)
        summed = jnp.dot(
            onehot,
            picked[tile * edges : (tile + 1) * edges, :].astype(jnp.bfloat16),
            preferred_element_type=jnp.float32,
        )
        rows = slice(tile * TILE, (tile + 1) * TILE)
        mix = (table[rows, :] + summed) / (1.0 + degree)
        mixed[rows, :] = mix
        top = jnp.maximum(jnp.max(jnp.abs(mix), 1, keepdims=True), 1e-30)
        step = jnp.clip(jnp.floor(8.0 * jnp.log2(top)) + (2.0 + SCALE_BIAS), 0.0, 255.0)
        code = jnp.round(mix * (jnp.exp2((SCALE_BIAS - step) * 0.125) * CODE_TOP))
        code = jnp.clip(code, -CODE_TOP, CODE_TOP - 1).astype(jnp.int32)
        codes[rows, :] = (code & (2**CODE_BITS - 1)) | (step.astype(jnp.int32) << CODE_BITS)

    lane = lax.broadcasted_iota(jnp.int32, (8, LANES), 1)
    row = lax.broadcasted_iota(jnp.int32, (8, LANES), 0)
    counted = jnp.where((lane == COARSE - 1) & (row == 0), live_count[0], 0)

    def pick_slots(block, side, coded):
        for slot in range(128):
            near = outbound.at[pl.ds(side * 128 + slot, outbound.shape[0] - 255)]
            coded[slot : slot + 1, :] = codes[pl.ds(near[block * 256], 1), :]

    def pack(peer, first, coded):
        to = peer * PACKED
        octet = [coded[first + 8 * k : first + 8 * k + 8, :] for k in range(8)]
        for k in range(4):
            low = (octet[k] >> 1) & 0xFFFF
            words[pl.ds(to + 8 * k, 8), :] = low | ((octet[k + 4] >> 1) << 16)
        fine = jnp.zeros((8, LANES), jnp.int32)
        coarse = counted
        for k in range(8):
            fine = fine | ((octet[k] & 1) << (4 * k + row // 2))
            scale = (octet[k] >> CODE_BITS) << (8 * (row // 2))
            coarse = coarse | jnp.where(lane == k, scale, 0)
        fine = jnp.where(lane < COARSE, coarse, fine)
        fine = fine | pltpu.roll(fine, 4, 0)
        fine = fine | pltpu.roll(fine, 2, 0)
        words[pl.ds(to + 32, 2), :] = fine[0:2, :]

    blocks = words.shape[0] // (4 * PACKED)
    pick_slots(0, 0, coded_even)

    def both(block, _):
        pick_slots(block, 1, coded_odd)
        pack(block * 4, 0, coded_even)
        pack(block * 4 + 1, 64, coded_even)
        pick_slots(jnp.minimum(block + 1, blocks - 1), 0, coded_even)
        pack(block * 4 + 2, 0, coded_odd)
        pack(block * 4 + 3, 64, coded_odd)
        return 0

    lax.fori_loop(0, blocks, both, 0)


def split_three(value):
    first = value.astype(jnp.bfloat16)
    rest = value - first.astype(jnp.float32)
    second = rest.astype(jnp.bfloat16)
    third = (rest - second.astype(jnp.float32)).astype(jnp.bfloat16)
    return first, second, third


def second_mix(
    core,
    live_count,
    sources,
    words,
    mixed,
    targets,
    w1_own,
    w1_other,
    b_own,
    b_other,
    w2_own,
    w2_other,
    embedded,
    sums,
    node_total,
    table,
    picked_even,
    picked_odd,
    w1,
    w2,
):
    local = mixed.shape[0]
    half = w1_own.shape[1]
    me = core[0]
    mine = pl.multiple_of(me * half, half)
    theirs = pl.multiple_of((1 - me) * half, half)
    for piece in range(3):
        w1[piece * LANES : (piece + 1) * LANES, 0:half] = w1_own[...]
        w1[piece * LANES : (piece + 1) * LANES, half : 2 * half] = w1_other[...]
    w2[0:half, 0:half] = w2_own[pl.ds(mine, half), :]
    w2[half : 2 * half, 0:half] = w2_own[pl.ds(theirs, half), :]
    w2[0:half, half : 2 * half] = w2_other[pl.ds(mine, half), :]
    w2[half : 2 * half, half : 2 * half] = w2_other[pl.ds(theirs, half), :]
    bias = jnp.concatenate([b_own[...], b_other[...]], 1)

    table[0:local, :] = mixed[...]

    lane = lax.broadcasted_iota(jnp.int32, (8, LANES), 1)
    row = lax.broadcasted_iota(jnp.int32, (8, LANES), 0)

    def unpack(peer):
        base = peer * PACKED
        to = pl.multiple_of(local + peer * 64, 64)
        pairs = [words[pl.ds(base + 8 * k, 8), :] for k in range(4)]
        rest = words[pl.ds(base + 26, 8), :]
        rest = jnp.where(row < 6, pltpu.roll(rest, 6, 0), rest)
        rest = jnp.where(row < 4, pltpu.roll(rest, 4, 0), rest)
        step = (rest >> (8 * (row // 2))) & 255
        scale = jnp.exp2((step.astype(jnp.float32) - SCALE_BIAS) * 0.125) * (1.0 / CODE_TOP)
        fine = jnp.where(lane < COARSE, 0, rest)
        for k in range(8):
            high = (pairs[k] << 16) >> 16 if k < 4 else pairs[k - 4] >> 16
            code = (high << 1) | ((fine >> (4 * k + row // 2)) & 1)
            table[pl.ds(to + 8 * k, 8), :] = code.astype(jnp.float32) * scale[:, k : k + 1]
        return rest

    def unpack_several(block, counts):
        for one in range(16):
            counts = counts + unpack(block * 16 + one)
        return counts

    counts = lax.fori_loop(
        0, words.shape[0] // (16 * PACKED), unpack_several, jnp.zeros((8, LANES), jnp.int32)
    )
    counts = jnp.where((lane == COARSE - 1) & (row == 0), counts, 0).astype(jnp.float32)
    counts = jnp.sum(jnp.sum(counts, 1, keepdims=True), 0, keepdims=True)
    node_total[...] = jnp.broadcast_to(counts, node_total.shape)
    edges = targets.shape[1]
    total = jnp.zeros((1, 2 * half), jnp.float32)
    squares = jnp.zeros((1, 2 * half), jnp.float32)

    def pick(tile, picked):
        picked[0:TILE, :] = mixed[tile * TILE : (tile + 1) * TILE, :]
        for edge in range(edges):
            source = sources[tile * edges + edge]
            picked[TILE + edge : TILE + edge + 1, :] = table[pl.ds(source, 1), :]

    pick(0, picked_even)
    for tile in range(local // TILE):
        rows = slice(tile * TILE, (tile + 1) * TILE)
        picked, later = (picked_even, picked_odd) if tile % 2 == 0 else (picked_odd, picked_even)
        if tile + 1 < local // TILE:
            pick(tile + 1, later)
        value = jnp.concatenate(split_three(picked[...]), 1)
        hidden = jnp.dot(value, w1[...], preferred_element_type=jnp.float32) + bias
        hidden = jnp.maximum(hidden, 0.0).astype(jnp.bfloat16)
        projected = jnp.dot(hidden, w2[...], preferred_element_type=jnp.float32)
        projected = projected.astype(jnp.bfloat16)
        onehot, degree = edge_table(targets, tile)
        summed = jnp.dot(onehot, projected[TILE:, :], preferred_element_type=jnp.float32)
        value = (projected[0:TILE, :].astype(jnp.float32) + summed) / (1.0 + degree)
        embedded[rows, :] = value
        slot = tile * TILE + lax.broadcasted_iota(jnp.int32, (TILE, 1), 0)
        value = jnp.where(slot < live_count[0], value, 0.0)
        total = total + jnp.sum(value, 0, keepdims=True)
        squares = squares + jnp.sum(value * value, 0, keepdims=True)
    for part in range(4):
        columns = slice(part * LANES, (part + 1) * LANES)
        for peer in range(sums.shape[0]):
            sums[peer, part : part + 1, :] = total[:, columns]
            sums[peer, part + 4 : part + 5, :] = squares[:, columns]


def add_and_copy(arrived, out):
    total = arrived[0]
    for peer in range(1, arrived.shape[0]):
        total = total + arrived[peer]
    for peer in range(out.shape[0]):
        out[peer] = total


def put_products(out, place, values):
    sides = [[values[8 * m : 8 * m + 8, side : side + LANES] for side in (0, LANES)] for m in range(4)]
    top = jnp.zeros((8, LANES), jnp.float32)
    for pair in sides:
        for side in pair:
            top = jnp.maximum(top, jnp.abs(side))
    top = jnp.maximum(jnp.max(top, 0, keepdims=True), 1e-30)
    step = jnp.floor(8.0 * jnp.log2(top)) + 2.0
    scale = jnp.exp2(step * -0.125) * 32767.0
    first = place * PRODUCTS
    for m, pair in enumerate(sides):
        low, high = (jnp.round(side * scale).astype(jnp.int32) for side in pair)
        out[first + 8 * m : first + 8 * m + 8, :] = (low & 0xFFFF) | (high << 16)
    out[first + 32 : first + 36, :] = jnp.broadcast_to(step.astype(jnp.int32), (4, LANES))


def sum_products(arrived):
    total = [[0.0, 0.0] for _ in range(4)]
    for place in range(arrived.shape[0] // PRODUCTS):
        first = place * PRODUCTS
        step = arrived[first + 32 : first + 33, :].astype(jnp.float32)
        scale = jnp.exp2(step * 0.125) * (1.0 / 32767.0)
        for m in range(4):
            word = arrived[first + 8 * m : first + 8 * m + 8, :]
            total[m][0] = total[m][0] + ((word << 16) >> 16).astype(jnp.float32) * scale
            total[m][1] = total[m][1] + (word >> 16).astype(jnp.float32) * scale
    return jnp.concatenate([jnp.concatenate(pair, 1) for pair in total], 0)


def add_products(arrived, out):
    total = sum_products(arrived)
    put_products(out, 0, total)
    for place in range(1, out.shape[0] // PRODUCTS):
        out[place * PRODUCTS : (place + 1) * PRODUCTS, :] = out[0:PRODUCTS, :]


def normalize(live_count, sums, node_total, embedded, out):
    total = node_total[...]
    scaled = jnp.sum(sums[...], 0) / total
    mean, square = scaled[0:4, :], scaled[4:8, :]
    dev = jnp.sqrt(square - mean * mean + 1e-05)
    slot = lax.broadcasted_iota(jnp.int32, (embedded.shape[0], 1), 0)
    live = slot < live_count[0]
    for part in range(4):
        columns = slice(part * LANES, (part + 1) * LANES)
        value = (embedded[:, columns] - mean[part : part + 1, :]) / dev[part : part + 1, :]
        out[:, columns] = jnp.where(live, value, 0.0).astype(jnp.bfloat16)


def correlate(core, own, other, normed, out):
    half = normed.shape[2]
    width = 2 * half
    groups, depth, wide = out.shape[0] // PRODUCTS, 8, 4
    contract = (((0,), (0,)), ((), ()))

    def give(left, right):
        product = lax.dot_general(left, right, contract, preferred_element_type=jnp.float32)
        for group in range(groups):
            rows = []
            for n1 in range(depth):
                first = ((group // wide) * depth * wide + n1 * wide + group % wide) * 4
                rows.append(product[first : first + 4, :])
            put_products(out, group, jnp.concatenate(rows, 0))

    @pl.when(core[0] == 0)
    def _():
        normed[0] = own[:, 0:half]
        normed[1] = other[:, half:width]
        give(own[...], other[:, half:width])

    @pl.when(core[0] == 1)
    def _():
        normed[0] = other[:, half:width]
        normed[1] = own[:, 0:half]
        give(other[...], own[:, 0:half])


def finish(core, node, arrived, node_total, correlation, loss):
    half = correlation.shape[1]
    share, depth, wide = 4, 8, 4
    n0, n1, n2 = node[0] // (depth * wide), (node[0] // wide) % depth, node[0] % wide
    value = sum_products(arrived) / node_total[0:1, 0:1]
    place = lax.broadcasted_iota(jnp.int32, value.shape, 0)
    row = ((n0 * depth + place // share) * wide + n2) * share + place % share
    column = lax.broadcasted_iota(jnp.int32, value.shape, 1) + core[0] * half
    mine = value[0:share, :]
    for other in range(1, depth):
        mine = jnp.where(n1 == other, value[other * share : (other + 1) * share, :], mine)
    correlation[...] = mine
    terms = jnp.where(row == column, jnp.square(1.0 - value), 0.005 * jnp.square(value))
    terms = jnp.sum(jnp.sum(terms, 1, keepdims=True), 0, keepdims=True)
    loss[...] = jnp.broadcast_to(terms[None], loss.shape)


def per_device(
    features, row_counts, send_rows, edge_src, edge_dst, edge_keep, w_first, b_first, w_second
):
    local, f_in = features.shape
    peers, halo = send_rows.shape[1], send_rows.shape[2]
    edges = edge_src.shape[1]
    tiles = local // TILE
    half = w_first.shape[1]
    width = 2 * half
    f32, bf16, i32 = jnp.float32, jnp.bfloat16, jnp.int32
    shape = jax.ShapeDtypeStruct
    core_index = lax.axis_index("feat")
    node_index = lax.axis_index(NODES)
    core = core_index.reshape(1).astype(i32)
    node = node_index.reshape(1).astype(i32)
    swap = [(0, 1), (1, 0)]
    planes, depth = lax.axis_size(PLANE), lax.axis_size("nodes_1")

    def partner(value):
        return lax.ppermute(value, "feat", swap)

    first_cores = [2 * peer for peer in range(peers)]
    second_cores = [
        2 * (four + peer) + 1 for four in reversed(range(0, peers, FOUR)) for peer in range(FOUR)
    ]

    def sum_over_nodes(blocks):
        blocks = lax.all_to_all(blocks, PLANE, split_axis=0, concat_axis=0, tiled=True)
        copies = call(
            add_and_copy, shape((depth, *blocks.shape[1:]), f32), [], blocks, name="add_sums"
        )
        return lax.all_to_all(copies, "nodes_1", split_axis=0, concat_axis=0, tiled=True)

    w1_other, w2_other = partner(w_first), partner(w_second)
    bias = b_first.reshape(1, half)
    bias_other = partner(bias)
    outbound = send_rows.reshape(peers * halo)
    sources = lax.dynamic_index_in_dim(edge_src, core_index, 0, False)
    targets = lax.dynamic_index_in_dim(edge_dst, core_index, 0, False)
    kept = lax.dynamic_index_in_dim(edge_keep, core_index, 0, False)
    targets = jnp.where(kept == 1, targets, -1).reshape(tiles, edges // tiles)

    rows_half = peers * halo // 2
    wide = features.astype(f32)
    sent = call(
        send_features,
        shape((rows_half, f_in), bf16),
        [pltpu.VMEM((rows_half, f_in), f32)],
        wide,
        scalars=(core, outbound),
        name="send_features",
    )
    sent, w1_other, w2_other, bias_other = lax.optimization_barrier(
        (sent, w1_other, w2_other, bias_other)
    )
    got = lax.all_to_all(
        sent.reshape(peers, halo // 2, f_in),
        NODES_FEAT,
        split_axis=0,
        concat_axis=0,
        axis_index_groups=[first_cores, second_cores],
        tiled=True,
    )
    got_other = partner(got)
    remote = sources - local
    slot_half = (remote % halo) // (halo // 2)
    from_other = (slot_half != core_index).astype(i32)
    sender = remote // halo
    sender = jnp.where(slot_half == 1, peers - FOUR - sender + 2 * (sender % FOUR), sender)
    remote = sender * (halo // 2) + remote % (halo // 2) + from_other * rows_half
    first_sources = jnp.where(sources < local, sources, remote + local)
    mixed, words = call(
        first_mix,
        (shape((local, f_in), f32), shape((peers * PACKED, f_in), i32)),
        [
            pltpu.VMEM((local + 2 * rows_half, f_in), f32),
            pltpu.VMEM((edges, f_in), f32),
            pltpu.VMEM((local, f_in), i32),
            pltpu.VMEM((2 * halo, f_in), i32),
            pltpu.VMEM((2 * halo, f_in), i32),
        ],
        wide,
        got.reshape(rows_half, f_in),
        got_other.reshape(rows_half, f_in),
        targets,
        scalars=(row_counts, first_sources, outbound),
        name="first_mix",
    )
    arrived = lax.all_to_all(
        words.reshape(peers * PACKED // 2, 2, f_in), NODES, split_axis=0, concat_axis=0, tiled=True
    )
    embedded, sums, node_total = call(
        second_mix,
        (
            shape((local, width), f32),
            shape((planes, 8, LANES), f32),
            shape((8, LANES), f32),
        ),
        [
            pltpu.VMEM((local + peers * halo, f_in), f32),
            pltpu.VMEM((TILE + edges // tiles, f_in), f32),
            pltpu.VMEM((TILE + edges // tiles, f_in), f32),
            pltpu.VMEM((3 * f_in, width), bf16),
            pltpu.VMEM((width, width), bf16),
        ],
        arrived.reshape(peers * PACKED, f_in),
        mixed,
        targets,
        w_first,
        w1_other,
        bias,
        bias_other,
        w_second,
        w2_other,
        scalars=(core, row_counts, sources),
        name="second_mix",
    )
    embedded_other = partner(embedded)
    sums = sum_over_nodes(sums)
    sums_other = partner(sums)

    def normalized(sums, embedded):
        return call(
            normalize,
            shape((local, width), bf16),
            [],
            sums,
            node_total,
            embedded,
            scalars=(row_counts,),
            name="normalize",
        )

    own, other = normalized(sums, embedded), normalized(sums_other, embedded_other)
    normed, partial = call(
        correlate,
        (shape((2, local, half), bf16), shape((planes * PRODUCTS, LANES), i32)),
        [],
        own,
        other,
        scalars=(core,),
        name="correlate",
    )
    partial = lax.all_to_all(
        partial.reshape(planes * PRODUCTS // 4, 4, LANES), PLANE, split_axis=0, concat_axis=0, tiled=True
    )
    partial = call(
        add_products,
        shape((depth * PRODUCTS, LANES), i32),
        [],
        partial.reshape(planes * PRODUCTS, LANES),
        name="add_products",
    )
    partial = lax.all_to_all(
        partial.reshape(depth * PRODUCTS // 4, 4, LANES), "nodes_1", split_axis=0, concat_axis=0, tiled=True
    )
    partial = partial.reshape(depth * PRODUCTS, LANES)
    devices = lax.axis_size(PLANE_FEAT)
    correlation, loss = call(
        finish,
        (shape((width // peers, half), f32), shape((devices, 1, LANES), f32)),
        [],
        partial,
        node_total,
        scalars=(core, node),
        name="finish",
    )
    losses = lax.all_to_all(loss, PLANE_FEAT, 0, 0, tiled=True)
    return (normed, correlation, jnp.sum(losses[:, 0, 0]))


def solution(mesh):
    torus = Mesh(
        mesh.devices.reshape(4, 8, 4, mesh.shape["feat"]), ("nodes_0", "nodes_1", "nodes_2", "feat")
    )
    placed = (
        P(NODES, None),
        P(NODES),
        P(NODES, None, None),
        P(None, NODES),
        P(None, NODES),
        P(None, NODES),
        P(None, "feat"),
        P("feat"),
        P(None, "feat"),
    )
    return jax.shard_map(
        per_device,
        mesh=torus,
        in_specs=placed,
        out_specs=(P(None, NODES, "feat"), P(NODES, "feat"), P()),
        check_vma=False,
    )
```
